256 devices in a mesh: groups: 2 (over z), ep: 16 (over y, core), rep: 8 (over x).
Axes of the slice: x: 8, y: 8, z: 2, core: 2. Of those that a mesh axis runs over, the one named last changes fastest.
The devices are a block of a 8x8x16 slice.
Arguments:
- prompt_hidden: bfloat16 [8, 384, 2048], P('groups', 'ep'), parts along dimension 0, may hold values from -6 to 6
- decode_hidden: bfloat16 [4096, 8, 2048], P(('groups', 'ep'), 'rep'), parts along dimension 0, may hold values from -6 to 6
- queries: bfloat16 [4096, 8, 2048], P(('groups', 'ep'), None, 'rep'), parts along dimension 0, may hold values from -128 to 128
- attn_gain: float32 [2048], replicated, may hold values from 0.1 to 1.9
- key_value_weight: bfloat16 [2048, 1024], P(None, 'rep'), may hold values from -0.125 to 0.125
- out_weight: bfloat16 [2048, 2048], P('rep'), may hold values from -0.5 to 0.5
- moe_gain: float32 [2048], replicated, may hold values from 0.1 to 1.9
- gate_weight: bfloat16 [128, 2048, 768], P(('ep', 'rep')), may hold values from -0.125 to 0.125
- up_weight: bfloat16 [128, 2048, 768], P(('ep', 'rep')), may hold values from -0.125 to 0.125
- down_weight: bfloat16 [128, 768, 2048], P(('ep', 'rep')), may hold values from -0.21875 to 0.21875
- expert_table: int32 [151936], replicated, may hold values from 0 to 127, as said below
- token_ids: int32 [2048, 8], P('ep', 'rep'), may hold values from 0 to 151935, as said below
- prompt_lengths: int32 [8], P('groups'), parts along dimension 0, may hold values from 1 to 384, 960 in all
Outputs:
- layer_out: bfloat16 [4096, 8, 2048], P(('groups', 'ep'), 'rep'), parts along dimension 0
The draws below stay inside these ranges and needn't reach their ends.
There are 2 independent parts, one for each index of `groups`. The reference program is written for one: setup_inputs(seed, part) draws one part's arguments, and reference() takes and returns one part's arrays. A program takes and returns all parts, laid end to end along the dimension named above; an argument that names none is the same for every part. Nothing has to cross between parts.
Inputs may be any that keep to these rules, and one draw needn't show every extreme that they name: `expert_table`: each expert is the value of exactly 1187 entries. `token_ids`: a device holds the 128 sequences of its index of ep at 8 // 8 steps of its index of rep; of these tokens at most 2 go to one expert; in every draw one expert receives exactly 2 from every device. `prompt_lengths`: the lengths of a group sum to 960 and the longest is 384.
All inputs are finite; a program needn't handle non-finite values.
Results may differ from the reference program's by a relative error of at most 0.017.
The reference program's roundings to bfloat16 on the way count: a program that leaves them out, or rounds other values in their place, can miss the bound.
Values may be sent and summed in bfloat16 or wider, within the bound.
A program may use at most 128 MiB of HBM per device.

```python
import math
import jax
import jax.numpy as jnp
import numpy as np
from jax import lax

MODEL_DIM = 2048
FF = 768
HEAD_DIM = 128
QUERY_HEADS = 16
KEY_VALUE_HEADS = 4
VOCAB = 151936
GROUP_PROMPTS = 4
PLEN = 384
DECODE_COUNT = 8
CAP = 2
SEQ_DEV = 128
SEQS = 2048
EXPERTS = 128
N_EP = 16
N_REP = 8


def hash_order(key):
    return jax.random.permutation(jax.random.fold_in(key, 7), VOCAB).astype(jnp.int32)


def draw_expert_table(key, part):
    return (hash_order(key) % EXPERTS).astype(jnp.int32)


def draw_token_ids(key, part):
    hash_perm = hash_order(key)
    inverse = jnp.zeros((VOCAB,), jnp.int32).at[hash_perm].set(jnp.arange(VOCAB, dtype=jnp.int32))
    ep_count = SEQS // SEQ_DEV
    rep_count = EXPERTS // ep_count
    step_rows = DECODE_COUNT // rep_count
    row_count = SEQ_DEV * step_rows
    blocks = EXPERTS
    slot_cols = EXPERTS * CAP
    key_hot, key_pick, key_place, key_token = jax.random.split(jax.random.fold_in(key, 13), 4)
    hot_expert = jax.random.randint(key_hot, (), 0, EXPERTS, dtype=jnp.int32)
    columns = jnp.arange(slot_cols, dtype=jnp.int32)
    column_expert = (columns // CAP).astype(jnp.int32)
    scores = jax.random.randint(key_pick, (blocks, slot_cols), 0, 1 << 20, dtype=jnp.int32) * slot_cols + columns[None, :]
    scores = jnp.where(column_expert[None, :] == hot_expert, 1 << 30, scores)
    picked_cols = lax.top_k(scores, row_count)[1].astype(jnp.int32)
    experts = jnp.take(column_expert, picked_cols)
    place_score = jax.random.randint(key_place, (blocks, row_count), 0, 1 << 20, dtype=jnp.int32) * row_count + jnp.arange(row_count, dtype=jnp.int32)[None, :]
    row_order = jnp.argsort(place_score, axis=1).astype(jnp.int32)
    experts = jnp.take_along_axis(experts, row_order, axis=1)
    within = jax.random.randint(key_token, (blocks, row_count), 0, VOCAB // EXPERTS, dtype=jnp.int32)
    token_rows = jnp.take(inverse, experts + EXPERTS * within)
    token_rows = token_rows.reshape(ep_count, rep_count, SEQ_DEV, step_rows).transpose(0, 2, 1, 3)
    return token_rows.reshape(SEQS, DECODE_COUNT).astype(jnp.int32)


def draw_queries(key, part):
    base_draw = jnp.clip(jax.random.normal(key, (SEQS, DECODE_COUNT, QUERY_HEADS, HEAD_DIM), jnp.float32), -4.0, 4.0)
    return base_draw.reshape(SEQS, DECODE_COUNT, QUERY_HEADS * HEAD_DIM).astype(jnp.bfloat16)


def levels(own_key, dims, cuts, low, top_value):
    def one(position, shards_of):
        steps = jax.random.uniform(jax.random.fold_in(jax.random.fold_in(own_key, 6), position), (shards_of,), jnp.float32, low / len(cuts), top_value / len(cuts))
        return jnp.repeat(jnp.exp(steps), dims[position] // shards_of).reshape((-1,) + (1,) * (len(dims) - position - 1))

    gain = one(*cuts[0])
    for cut in cuts[1:]:
        gain = gain * one(*cut)
    return gain


def profile(count, total, bound, skew):
    loads = [(1 << 20) // math.isqrt(standing ** skew) + 1 for standing in range(2, count + 1)]
    spare, holding = total - bound - (count - 1), [1] * (count - 1)
    while spare > 0:
        movable = [i for i in range(count - 1) if holding[i] < bound]
        whole, left = sum([loads[i] for i in movable]), spare
        for i in movable:
            addition = min(bound - holding[i], max(1, left * loads[i] // whole), spare)
            holding[i] = holding[i] + addition
            spare = spare - addition
    return np.array([bound] + holding)


def uneven_parts(rng, count, total, reach, skew):
    if count == 2:
        one = jax.random.randint(rng, (), max(1, total - reach), min(reach, total - 1) + 1)
        return jnp.stack([one, total - one])
    sizes = jnp.asarray(profile(count, total, reach, skew), jnp.int32)
    couples = (count - 1) // 2
    donor, sink = sizes[1:1 + 2 * couples:2], sizes[2:2 + 2 * couples:2]
    margin = jnp.minimum(donor - 1, reach - sink)
    moved = jax.random.randint(jax.random.fold_in(rng, 1), (couples,), 0, 1 << 20) % (margin + 1)
    sizes = sizes.at[1:1 + 2 * couples:2].set(donor - moved).at[2:2 + 2 * couples:2].set(sink + moved)
    return sizes[jax.random.permutation(jax.random.fold_in(rng, 2), count)]


def bell_draw(own_key, shape, deviation, reach, cuts=(), kind=jnp.bfloat16):
    gain = levels(own_key, shape, cuts, -0.22, 0.18) if cuts else 1.0
    values = jax.random.normal(own_key, shape, jnp.float32) * deviation * gain
    return jnp.minimum(jnp.maximum(values, -reach), reach).astype(kind)


def setup_inputs(seed: int = 0, part: int = 0) -> dict:
    key_of = jax.random.split(jax.random.key(seed), 14)
    part_splits = jax.random.split(jax.random.fold_in(key_of[13], part), 14)
    prompt_hidden = bell_draw(part_splits[0], (GROUP_PROMPTS, PLEN, MODEL_DIM), 1.0, 6.0, ((1, 16),))
    decode_hidden = bell_draw(part_splits[1], (SEQS, DECODE_COUNT, MODEL_DIM), 1.0, 6.0, ((0, 16), (1, 8)))
    queries = draw_queries(jax.random.fold_in(jax.random.fold_in(key_of[13], part), 71), part)
    attn_gain = jnp.clip(1.0 + 0.18 * jax.random.normal(key_of[3], (MODEL_DIM,), jnp.float32), 0.1, 1.9)
    key_value_weight = bell_draw(key_of[4], (MODEL_DIM, KEY_VALUE_HEADS * 2 * HEAD_DIM), MODEL_DIM ** -0.5, 0.125, ((1, 8),))
    out_weight = bell_draw(key_of[5], (QUERY_HEADS * HEAD_DIM, MODEL_DIM), (QUERY_HEADS * HEAD_DIM // 16) ** -0.5, 0.5, ((0, 8),))
    moe_gain = jnp.clip(1.0 + 0.18 * jax.random.normal(key_of[6], (MODEL_DIM,), jnp.float32), 0.1, 1.9)
    gate_weight = bell_draw(key_of[7], (EXPERTS, MODEL_DIM, FF), MODEL_DIM ** -0.5, 0.125, ((0, 128),))
    up_weight = bell_draw(key_of[8], (EXPERTS, MODEL_DIM, FF), MODEL_DIM ** -0.5, 0.125, ((0, 128),))
    down_weight = bell_draw(key_of[9], (EXPERTS, FF, MODEL_DIM), FF ** -0.5, 0.21875, ((0, 128),))
    expert_table = draw_expert_table(jax.random.fold_in(key_of[13], 71), part)
    token_ids = draw_token_ids(jax.random.fold_in(key_of[13], 71), part)
    prompt_lengths = uneven_parts(part_splits[12], GROUP_PROMPTS, 5 * PLEN // 2, PLEN, 1).astype(jnp.int32)
    return dict(prompt_hidden=prompt_hidden, decode_hidden=decode_hidden, queries=queries, attn_gain=attn_gain, key_value_weight=key_value_weight, out_weight=out_weight, moe_gain=moe_gain, gate_weight=gate_weight, up_weight=up_weight, down_weight=down_weight, expert_table=expert_table, token_ids=token_ids, prompt_lengths=prompt_lengths)


EPS = 1e-06
THETA = 1000000.0

def rms_scale(hidden, gain_vec):
    widened = hidden.astype(jnp.float32)
    mean_sq = lax.optimization_barrier(jnp.mean(widened * widened, axis=-1, keepdims=True))
    return widened * lax.rsqrt(mean_sq + EPS) * gain_vec

def rotate(vectors, positions):
    half_dim = vectors.shape[-1] // 2
    inverse_freq = jnp.exp(jnp.arange(half_dim, dtype=jnp.float32) * (-2.0 * math.log(THETA) / vectors.shape[-1]))
    angles = positions[..., None] * inverse_freq
    cosine = jnp.cos(angles)
    sine_part = jnp.sin(angles)
    first_half = vectors[..., :half_dim]
    second_half = vectors[..., half_dim:]
    return jnp.concatenate([first_half * cosine - second_half * sine_part, second_half * cosine + first_half * sine_part], axis=-1)

def project_kv(hidden, gain_vec, key_value_weight, positions):
    leading = hidden.shape[:-1]
    normed = rms_scale(hidden, gain_vec).astype(jnp.bfloat16)
    kv_pairs = jnp.dot(normed.reshape(-1, hidden.shape[-1]), key_value_weight, preferred_element_type=jnp.float32)
    kv_pairs = kv_pairs.reshape(leading + (key_value_weight.shape[1] // (2 * HEAD_DIM), 2, HEAD_DIM))
    key_part = rotate(kv_pairs[..., 0, :], positions[..., None]).astype(jnp.bfloat16)
    value_part = kv_pairs[..., 1, :].astype(jnp.bfloat16)
    return (key_part, value_part)

def reference(prompt_hidden, decode_hidden, queries, attn_gain, key_value_weight, out_weight, moe_gain, gate_weight, up_weight, down_weight, expert_table, token_ids, prompt_lengths):
    samples = SEQS // GROUP_PROMPTS
    prompt_pos = jnp.broadcast_to(jnp.arange(PLEN, dtype=jnp.float32)[None, :], (GROUP_PROMPTS, PLEN))
    prompt_keys, prompt_values = project_kv(prompt_hidden, attn_gain, key_value_weight, prompt_pos)
    prompt_of = (jnp.arange(SEQS, dtype=jnp.int32) // samples).astype(jnp.int32)
    lengths = jnp.take(prompt_lengths, prompt_of)
    decode_pos = lengths[:, None].astype(jnp.float32) + jnp.arange(DECODE_COUNT, dtype=jnp.float32)[None, :]
    decode_keys, decode_values = project_kv(decode_hidden, attn_gain, key_value_weight, decode_pos)
    group_count = QUERY_HEADS // KEY_VALUE_HEADS
    score_scale = HEAD_DIM ** (-0.5)
    key_pos = jnp.arange(PLEN, dtype=jnp.int32)
    causal = jnp.arange(DECODE_COUNT)[None, :] <= jnp.arange(DECODE_COUNT)[:, None]
    self_mask = causal[:, None, None, :]

    def attend(sequence_index):
        query_matrix = queries[sequence_index].astype(jnp.float32).reshape(DECODE_COUNT, KEY_VALUE_HEADS, group_count, HEAD_DIM)
        prompt = prompt_of[sequence_index]
        cache_keys = prompt_keys[prompt].astype(jnp.float32)
        cache_values = prompt_values[prompt].astype(jnp.float32)
        key_valid = key_pos < lengths[sequence_index]
        cache_scores = jnp.einsum('tkgd,nkd->tkgn', query_matrix, cache_keys) * score_scale
        self_scores = jnp.einsum('tkgd,ukd->tkgu', query_matrix, decode_keys[sequence_index].astype(jnp.float32)) * score_scale
        cache_scores = jnp.where(key_valid, cache_scores, -1e+30)
        self_scores = jnp.where(self_mask, self_scores, -1e+30)
        row_top = jnp.maximum(lax.optimization_barrier(jnp.max(cache_scores, axis=-1)), lax.optimization_barrier(jnp.max(self_scores, axis=-1)))
        cache_weights = jnp.where(key_valid, jnp.exp(cache_scores - row_top[..., None]), 0.0)
        self_weights = jnp.where(self_mask, jnp.exp(self_scores - row_top[..., None]), 0.0)
        row_total = lax.optimization_barrier(jnp.sum(cache_weights, axis=-1)) + lax.optimization_barrier(jnp.sum(self_weights, axis=-1))
        numerator = jnp.einsum('tkgn,nkd->tkgd', cache_weights.astype(jnp.bfloat16).astype(jnp.float32), cache_values)
        numerator = numerator + jnp.einsum('tkgu,ukd->tkgd', self_weights.astype(jnp.bfloat16).astype(jnp.float32), decode_values[sequence_index].astype(jnp.float32))
        return (numerator / row_total[..., None]).reshape(DECODE_COUNT, QUERY_HEADS * HEAD_DIM).astype(jnp.bfloat16)
    attended = lax.map(attend, jnp.arange(SEQS, dtype=jnp.int32))
    projected = jnp.dot(attended.reshape(SEQS * DECODE_COUNT, QUERY_HEADS * HEAD_DIM), out_weight, preferred_element_type=jnp.float32).reshape(SEQS, DECODE_COUNT, MODEL_DIM)
    attn_mixed = (decode_hidden.astype(jnp.float32) + projected).astype(jnp.bfloat16)
    normed = rms_scale(attn_mixed, moe_gain).astype(jnp.bfloat16).reshape(SEQS * DECODE_COUNT, MODEL_DIM)
    chosen = jnp.take(expert_table, token_ids.reshape(-1)).astype(jnp.int32)
    row_total_count = SEQS * DECODE_COUNT
    per_expert = CAP * N_EP * N_REP

    def run_expert(collected, expert):
        row_index = jnp.nonzero(chosen == expert, size=per_expert, fill_value=row_total_count)[0].astype(jnp.int32)
        token_rows = jnp.take(normed, row_index, axis=0, mode='fill', fill_value=0)
        gate_proj = jnp.dot(token_rows, gate_weight[expert], preferred_element_type=jnp.float32)
        up_proj = jnp.dot(token_rows, up_weight[expert], preferred_element_type=jnp.float32)
        hidden = (jax.nn.silu(gate_proj) * up_proj).astype(jnp.bfloat16)
        result = jnp.dot(hidden, down_weight[expert], preferred_element_type=jnp.float32).astype(jnp.bfloat16)
        return (collected.at[row_index].set(result, mode='drop'), None)
    expert_out, unused = lax.scan(run_expert, jnp.zeros((row_total_count, MODEL_DIM), jnp.bfloat16), jnp.arange(EXPERTS, dtype=jnp.int32))
    layer_out = (attn_mixed.astype(jnp.float32) + expert_out.astype(jnp.float32).reshape(SEQS, DECODE_COUNT, MODEL_DIM)).astype(jnp.bfloat16)
    return layer_out
```

```python
import functools
import math

import jax
import jax.numpy as jnp
from jax import lax
from jax.experimental import pallas as pl
from jax.experimental.pallas import tpu as pltpu
from jax.sharding import PartitionSpec as P

HEAD_DIM = 128
QUERY_HEADS = 16
KEY_VALUE_HEADS = 4
GROUP_PROMPTS = 4
CAP = 2

EPS = 1e-06
THETA = 1000000.0
MESH = pl.DeviceIdType.MESH
F32 = jnp.float32
BF16 = jnp.bfloat16


def in_one_piece(arrays, axis, dim, along):
    both = jnp.concatenate(arrays, axis=along)
    filled, at, outs = (lax.all_gather(both, axis, axis=dim, tiled=True), 0, [])
    for a in arrays:
        outs.append(lax.slice_in_dim(filled, at, at + a.shape[along], axis=along))
        at += a.shape[along]
    return tuple(outs)


def swapped(block, axis, bit):
    count = lax.axis_size(axis)
    route = []
    for low in range(count):
        high = low | 1 << bit
        if high != low and high < count:
            route += [(low, high), (high, low)]
    return lax.ppermute(block, axis, route)


def rms_scale(hidden, gain_vec):
    widened = hidden.astype(F32)
    mean_sq = jnp.mean(widened * widened, axis=-1, keepdims=True)
    return widened * lax.rsqrt(mean_sq + EPS) * gain_vec


def rotate(vectors, positions):
    half_dim = vectors.shape[-1] // 2
    inverse_freq = jnp.exp(
        jnp.arange(half_dim, dtype=F32) * (-2.0 * math.log(THETA) / vectors.shape[-1])
    )
    angles = positions[..., None] * inverse_freq
    cosine = jnp.cos(angles)
    sine_part = jnp.sin(angles)
    first_half = vectors[..., :half_dim]
    second_half = vectors[..., half_dim:]
    return jnp.concatenate(
        [
            first_half * cosine - second_half * sine_part,
            second_half * cosine + first_half * sine_part,
        ],
        axis=-1,
    )


def dot(a, b):
    return jnp.dot(a, b, preferred_element_type=F32)


def dot_t(a, b):
    return lax.dot_general(a, b, (((0,), (0,)), ((), ())), preferred_element_type=F32)


def one_hot(hit):
    return jnp.where(hit, 1.0, 0.0).astype(BF16)


def moe_kernel(
    nx, ne, mixed_ref, gain_ref, row_ref, col_ref, gate_hbm, up_hbm, down_hbm, out_ref,
    gate, up, down, normed, xin, hid,
    s0, s1, r0, r1, t0, t1, q0, q1, o0, o1, b0, b1, c0, c1, f0, f1,
    wsem, ssem, rsem,
):
    e, x, g = lax.axis_index("ep"), lax.axis_index("rep"), lax.axis_index("groups")
    rows, width = mixed_ref.shape
    ff = gate.shape[1]
    half = nx * ne
    loads = [
        pltpu.make_async_copy(gate_hbm, gate, wsem.at[0]),
        pltpu.make_async_copy(up_hbm, up, wsem.at[1]),
        pltpu.make_async_copy(down_hbm, down, wsem.at[2]),
    ]
    for load in loads:
        load.start()
    barrier = pltpu.get_barrier_semaphore()
    for i in range(1, nx):
        peer = (g, e, lax.rem(x + i, nx))
        pl.semaphore_signal(barrier, inc=1, device_id=peer, device_id_type=MESH)
    for i in range(1, ne):
        peer = (g, lax.rem(e + i, ne), x)
        pl.semaphore_signal(barrier, inc=1, device_id=peer, device_id_type=MESH)

    widened = mixed_ref[...].astype(F32)
    scale = lax.rsqrt(jnp.mean(widened * widened, axis=-1, keepdims=True) + EPS)
    normed[...] = (widened * scale * gain_ref[...]).astype(BF16)

    row, col = row_ref[...], col_ref[...]
    first = lax.broadcasted_iota(jnp.int32, (rows, rows), 0)
    second = lax.broadcasted_iota(jnp.int32, (rows, rows), 1)
    earlier = jnp.where((row == col) & (first < second), 1, 0)
    rank = jnp.sum(earlier, axis=0, keepdims=True)
    slot = lax.broadcasted_iota(jnp.int32, (half, rows), 0)
    turned = lax.rem(slot, ne) * nx + slot // ne
    pick0 = one_hot((turned == row) & (rank == 0))
    pick1 = one_hot((slot == row) & (rank == 1))

    here = lax.broadcasted_iota(jnp.int32, (half, half), 0)
    there = lax.broadcasted_iota(jnp.int32, (half, half), 1)
    to_ex = one_hot(there == lax.rem(here, nx) * ne + here // nx)
    to_xe = one_hot(there == lax.rem(here, ne) * nx + here // ne)

    tile = 512

    def over_columns(body):
        def step(i, carry):
            body(pl.ds(pl.multiple_of(i * tile, tile), tile))
            return carry

        lax.fori_loop(0, width // tile, step, 0)

    def put(ref, cols, value):
        ref[:, :, cols] = value.reshape(ref.shape[0], ref.shape[1], tile).astype(BF16)

    def get(ref, cols):
        return ref[:, :, cols].astype(F32).reshape(half, tile).astype(BF16)

    def send_x(src, dst, k):
        for i in range(1, nx):
            to = lax.rem(x + i, nx)
            pltpu.make_async_remote_copy(
                src.at[to], dst.at[x], ssem.at[k], rsem.at[k],
                device_id=(g, e, to), device_id_type=MESH,
            ).start()

    def send_e(src, dst, k):
        for i in range(1, ne):
            to = lax.rem(e + i, ne)
            pltpu.make_async_remote_copy(
                src.at[to], dst.at[e], ssem.at[k], rsem.at[k],
                device_id=(g, to, x), device_id_type=MESH,
            ).start()

    def arrive(src, dst, k):
        n = dst.shape[0] - 1
        pltpu.make_async_copy(src.at[pl.ds(0, n)], dst.at[pl.ds(0, n)], ssem.at[k]).wait()
        pltpu.make_async_copy(src.at[pl.ds(0, n)], dst.at[pl.ds(0, n)], rsem.at[k]).wait()

    def scatter(cols):
        put(s0, cols, dot(pick0, normed[:, cols]))
        put(s1, cols, dot(pick1, normed[:, cols]))

    over_columns(scatter)
    pl.semaphore_wait(barrier, nx + ne - 2)
    send_x(s0, r0, 0)
    send_e(s1, r1, 1)
    r0[x] = s0[x]
    r1[e] = s1[e]
    arrive(s0, r0, 0)
    over_columns(lambda cols: put(t0, cols, dot(to_ex, get(r0, cols))))
    send_e(t0, q0, 2)
    q0[e] = t0[e]
    arrive(s1, r1, 1)
    over_columns(lambda cols: put(t1, cols, dot(to_xe, get(r1, cols))))
    send_x(t1, q1, 3)
    q1[x] = t1[x]

    for load in loads:
        load.wait()
    arrive(t0, q0, 2)
    arrive(t1, q1, 3)

    def collect(cols):
        xin[pl.ds(0, half), cols] = get(q0, cols)
        xin[pl.ds(half, half), cols] = get(q1, cols)

    over_columns(collect)
    ftile = 256

    def inner(i, carry):
        cols = pl.ds(pl.multiple_of(i * ftile, ftile), ftile)
        gate_proj = dot(xin[...], gate[:, cols])
        up_proj = dot(xin[...], up[:, cols])
        hid[:, cols] = (jax.nn.silu(gate_proj) * up_proj).astype(BF16)
        return carry

    lax.fori_loop(0, ff // ftile, inner, 0)

    def outer(cols):
        put(o0, cols, dot(hid[pl.ds(0, half), :], down[:, cols]))
        put(o1, cols, dot(hid[pl.ds(half, half), :], down[:, cols]))

    over_columns(outer)
    send_e(o0, b0, 4)
    send_x(o1, b1, 5)
    b0[e] = o0[e]
    b1[x] = o1[x]
    arrive(o0, b0, 4)
    over_columns(lambda cols: put(c0, cols, dot(to_xe, get(b0, cols))))
    send_x(c0, f0, 6)
    f0[x] = c0[x]
    arrive(o1, b1, 5)
    over_columns(lambda cols: put(c1, cols, dot(to_ex, get(b1, cols))))
    send_e(c1, f1, 7)
    f1[e] = c1[e]
    arrive(c0, f0, 6)
    arrive(c1, f1, 7)

    def combine(cols):
        moe = dot_t(pick0, get(f0, cols)) + dot_t(pick1, get(f1, cols))
        out_ref[:, cols] = (mixed_ref[:, cols].astype(F32) + moe).astype(BF16)

    over_columns(combine)


def moe(mixed, gain, chosen, gate_weight, up_weight, down_weight):
    nx, ne = lax.axis_size("rep"), lax.axis_size("ep")
    rows, width = mixed.shape
    ff = gate_weight.shape[2]
    half = nx * ne
    xe = pltpu.VMEM((nx, ne, width), BF16)
    ex = pltpu.VMEM((ne, nx, width), BF16)
    vmem, any_ = pl.BlockSpec(memory_space=pltpu.VMEM), pl.BlockSpec(memory_space=pl.ANY)
    return pl.pallas_call(
        functools.partial(moe_kernel, nx, ne),
        out_shape=jax.ShapeDtypeStruct((rows, width), BF16),
        in_specs=[vmem] * 4 + [any_] * 3,
        out_specs=vmem,
        scratch_shapes=[
            pltpu.VMEM((width, ff), BF16), pltpu.VMEM((width, ff), BF16), pltpu.VMEM((ff, width), BF16),
            pltpu.VMEM((rows, width), BF16), pltpu.VMEM((2 * half, width), BF16), pltpu.VMEM((2 * half, ff), BF16),
            xe, ex, xe, ex, ex, xe, ex, xe, ex, xe, ex, xe, xe, ex, xe, ex,
            pltpu.SemaphoreType.DMA((3,)), pltpu.SemaphoreType.DMA((8,)), pltpu.SemaphoreType.DMA((8,)),
        ],
        compiler_params=pltpu.CompilerParams(
            collective_id=1, has_side_effects=True, vmem_limit_bytes=48 << 20
        ),
        name="moe",
    )(
        mixed, gain.reshape(1, width), chosen.reshape(1, rows), chosen.reshape(rows, 1),
        gate_weight[0], up_weight[0], down_weight[0],
    )


def local(
    prompt_hidden,
    decode_hidden,
    queries,
    attn_gain,
    key_value_weight,
    out_weight,
    moe_gain,
    gate_weight,
    up_weight,
    down_weight,
    expert_table,
    token_ids,
    prompt_lengths,
):
    full_hidden = lax.all_gather(decode_hidden, "rep", axis=1, tiled=True)
    sequences_local, steps_total, model_width = full_hidden.shape
    prompt_length_local = prompt_hidden.shape[1]
    qh_dev = queries.shape[2] // HEAD_DIM
    group_count = QUERY_HEADS // KEY_VALUE_HEADS
    ep_count = lax.axis_size("ep")
    rep_count = lax.axis_size("rep")
    ep_index = lax.axis_index("ep")
    rep_index = lax.axis_index("rep")
    seq_total = sequences_local * ep_count
    samples = seq_total // GROUP_PROMPTS
    score_scale = HEAD_DIM ** (-0.5)
    step_rows = steps_total // rep_count
    blocks = key_value_weight.shape[1] // HEAD_DIM

    def own_columns(hidden, positions):
        leading = hidden.shape[:-1]
        normed = rms_scale(hidden, attn_gain).astype(BF16)
        projected = jnp.dot(
            normed.reshape(-1, model_width), key_value_weight, preferred_element_type=F32
        )
        projected = projected.reshape(leading + (blocks, HEAD_DIM))
        block_ids = rep_index * blocks + jnp.arange(blocks, dtype=jnp.int32)
        is_key = (block_ids % 2 == 0)[:, None]
        turned = rotate(projected, positions[..., None])
        return (
            jnp.where(is_key, turned, projected)
            .astype(BF16)
            .reshape(leading + (blocks * HEAD_DIM,))
        )

    key_pos = ep_index * prompt_length_local + jnp.arange(prompt_length_local, dtype=jnp.int32)
    prompt_pos = jnp.broadcast_to(
        key_pos.astype(F32)[None, :], (GROUP_PROMPTS, prompt_length_local)
    )
    own_seqs = ep_index * sequences_local + jnp.arange(sequences_local, dtype=jnp.int32)
    own_prompt = own_seqs // samples
    own_lengths = jnp.take(prompt_lengths, own_prompt)
    decode_pos = (
        own_lengths[:, None].astype(F32)
        + jnp.arange(steps_total, dtype=F32)[None, :]
    )
    prompt_part = own_columns(prompt_hidden, prompt_pos)
    decode_part = own_columns(full_hidden, decode_pos)
    prompt_hot = own_prompt[:, None] == jnp.arange(GROUP_PROMPTS, dtype=jnp.int32)[None, :]
    partner_prompt, partner_decode = swapped((prompt_part, decode_part), "rep", 0)
    holds_key = rep_index % 2 == 0
    prompt_columns = jnp.where(
        holds_key,
        jnp.concatenate([prompt_part, partner_prompt], axis=2),
        jnp.concatenate([partner_prompt, prompt_part], axis=2),
    )
    decode_columns = jnp.where(
        holds_key,
        jnp.concatenate([decode_part, partner_decode], axis=2),
        jnp.concatenate([partner_decode, decode_part], axis=2),
    )
    heads_here = 1
    head_base = rep_index // 2
    prompt_key_value = prompt_columns.reshape(
        GROUP_PROMPTS, prompt_length_local, heads_here, 2, HEAD_DIM
    )
    decode_key_value = decode_columns.reshape(sequences_local, steps_total, heads_here, 2, HEAD_DIM)
    prompt_keys = prompt_key_value[:, :, :, 0, :]
    prompt_values = prompt_key_value[:, :, :, 1, :]
    decode_keys = decode_key_value[:, :, :, 0, :]
    decode_values = decode_key_value[:, :, :, 1, :]
    query_matrix = queries.reshape(sequences_local, steps_total, qh_dev, HEAD_DIM)
    head_pick = (
        rep_index * qh_dev + jnp.arange(qh_dev, dtype=jnp.int32)
    ) // group_count - head_base
    own_keys = jnp.take(decode_keys, head_pick, axis=2)
    own_values = jnp.take(decode_values, head_pick, axis=2)
    self_scores = (
        jnp.einsum("sthd,suhd->sthu", query_matrix, own_keys, preferred_element_type=F32)
        * score_scale
    )
    self_mask = (
        jnp.arange(steps_total, dtype=jnp.int32)[None, :]
        <= jnp.arange(steps_total, dtype=jnp.int32)[:, None]
    )[None, :, None, :]
    self_scores = jnp.where(self_mask, self_scores, -1e30)
    self_top = jnp.max(self_scores, axis=-1)
    start_weights = jnp.where(self_mask, jnp.exp(self_scores - self_top[..., None]), 0.0)
    pieces = in_one_piece((prompt_keys, prompt_values), "ep", 1, 0)
    row_top = self_top
    row_total = jnp.sum(start_weights, axis=-1)
    weighted = jnp.einsum(
        "sthu,suhd->sthd",
        start_weights.astype(BF16),
        own_values,
        preferred_element_type=F32,
    )
    piece_keys = jnp.take(pieces[0], head_pick, axis=2)
    piece_values = jnp.take(pieces[1], head_pick, axis=2)
    piece_len = piece_keys.shape[1]
    valid = jnp.arange(piece_len, dtype=jnp.int32)[None, :] < prompt_lengths[:, None]
    key_mask = prompt_hot[:, None, None, :, None] & valid[None, None, None, :, :]
    scores = (
        jnp.einsum("sthd,pnhd->sthpn", query_matrix, piece_keys, preferred_element_type=F32)
        * score_scale
    )
    scores = jnp.where(key_mask, scores, -1e30)
    new_top = jnp.maximum(row_top, jnp.max(scores, axis=(-2, -1)))
    decay = jnp.exp(row_top - new_top)
    weights = jnp.where(key_mask, jnp.exp(scores - new_top[..., None, None]), 0.0)
    weighted = weighted * decay[..., None] + jnp.einsum(
        "sthpn,pnhd->sthd",
        weights.astype(BF16),
        piece_values,
        preferred_element_type=F32,
    )
    row_top, row_total, weighted = (
        new_top,
        row_total * decay + jnp.sum(weights, axis=(-2, -1)),
        weighted,
    )
    attended = weighted / row_total[..., None]
    heads_out = attended.reshape(sequences_local, steps_total, qh_dev * HEAD_DIM).astype(
        BF16
    )
    by_step = jnp.swapaxes(heads_out, 0, 1)
    attn_sum = jnp.swapaxes(
        lax.psum_scatter(
            jnp.dot(
                by_step.reshape(-1, by_step.shape[-1]),
                out_weight,
                preferred_element_type=F32,
            )
            .reshape(step_rows * lax.axis_size("rep"), sequences_local, model_width)
            .astype(BF16),
            "rep",
            scatter_dimension=0,
            tiled=True,
        ).astype(F32),
        0,
        1,
    )
    attn_mixed = (decode_hidden.astype(F32) + attn_sum).astype(BF16)
    row_count = sequences_local * step_rows
    chosen = jnp.take(expert_table, token_ids.reshape(row_count))
    out = moe(
        attn_mixed.reshape(row_count, model_width), moe_gain, chosen, gate_weight, up_weight, down_weight
    )
    return out.reshape(sequences_local, step_rows, model_width)


def solution(mesh):
    placed = (
        P("groups", "ep", None),
        P(("groups", "ep"), "rep", None),
        P(("groups", "ep"), None, "rep"),
        P(),
        P(None, "rep"),
        P("rep", None),
        P(),
        P(("ep", "rep"), None, None),
        P(("ep", "rep"), None, None),
        P(("ep", "rep"), None, None),
        P(),
        P("ep", "rep"),
        P("groups"),
    )
    return jax.shard_map(
        local,
        mesh=mesh,
        in_specs=placed,
        out_specs=P(("groups", "ep"), "rep", None),
        check_vma=False,
    )
```

```python
import functools
import math

import jax
import jax.numpy as jnp
from jax import lax
from jax.experimental import pallas as pl
from jax.experimental.pallas import tpu as pltpu
from jax.sharding import PartitionSpec as P

HEAD_DIM = 128
QUERY_HEADS = 16
KEY_VALUE_HEADS = 4
GROUP_PROMPTS = 4
CAP = 2

EPS = 1e-06
THETA = 1000000.0
MESH = pl.DeviceIdType.MESH
F32 = jnp.float32
BF16 = jnp.bfloat16


def dot(a, b):
    return jnp.dot(a, b, preferred_element_type=F32)


def dot_t(a, b):
    return lax.dot_general(a, b, (((0,), (0,)), ((), ())), preferred_element_type=F32)


def one_hot(hit):
    return jnp.where(hit, 1.0, 0.0).astype(BF16)


def moe_kernel(
    nx, ne, mixed_ref, gain_ref, row_ref, col_ref, gate_hbm, up_hbm, down_hbm, out_ref,
    gate, up, down, normed, xin, hid,
    s0, s1, r0, r1, t0, t1, q0, q1, o0, o1, b0, b1, c0, c1, f0, f1,
    wsem, ssem, rsem,
):
    e, x, g = lax.axis_index("ep"), lax.axis_index("rep"), lax.axis_index("groups")
    rows, width = mixed_ref.shape
    ff = gate.shape[1]
    half = nx * ne
    loads = [
        pltpu.make_async_copy(gate_hbm, gate, wsem.at[0]),
        pltpu.make_async_copy(up_hbm, up, wsem.at[1]),
        pltpu.make_async_copy(down_hbm, down, wsem.at[2]),
    ]
    for load in loads:
        load.start()
    barrier = pltpu.get_barrier_semaphore()
    for i in range(1, nx):
        peer = (g, e, lax.rem(x + i, nx))
        pl.semaphore_signal(barrier, inc=1, device_id=peer, device_id_type=MESH)
    for i in range(1, ne):
        peer = (g, lax.rem(e + i, ne), x)
        pl.semaphore_signal(barrier, inc=1, device_id=peer, device_id_type=MESH)

    widened = mixed_ref[...].astype(F32)
    scale = lax.rsqrt(jnp.mean(widened * widened, axis=-1, keepdims=True) + EPS)
    normed[...] = (widened * scale * gain_ref[...]).astype(BF16)

    row, col = row_ref[...], col_ref[...]
    first = lax.broadcasted_iota(jnp.int32, (rows, rows), 0)
    second = lax.broadcasted_iota(jnp.int32, (rows, rows), 1)
    earlier = jnp.where((row == col) & (first < second), 1, 0)
    rank = jnp.sum(earlier, axis=0, keepdims=True)
    slot = lax.broadcasted_iota(jnp.int32, (half, rows), 0)
    turned = lax.rem(slot, ne) * nx + slot // ne
    pick0 = one_hot((turned == row) & (rank == 0))
    pick1 = one_hot((slot == row) & (rank == 1))

    here = lax.broadcasted_iota(jnp.int32, (half, half), 0)
    there = lax.broadcasted_iota(jnp.int32, (half, half), 1)
    to_ex = one_hot(there == lax.rem(here, nx) * ne + here // nx)
    to_xe = one_hot(there == lax.rem(here, ne) * nx + here // ne)

    tile = 512

    def over_columns(body):
        def step(i, carry):
            body(pl.ds(pl.multiple_of(i * tile, tile), tile))
            return carry

        lax.fori_loop(0, width // tile, step, 0)

    def put(ref, cols, value):
        ref[:, :, cols] = value.reshape(ref.shape[0], ref.shape[1], tile).astype(BF16)

    def get(ref, cols):
        return ref[:, :, cols].astype(F32).reshape(half, tile).astype(BF16)

    def send_x(src, dst, k):
        for i in range(1, nx):
            to = lax.rem(x + i, nx)
            pltpu.make_async_remote_copy(
                src.at[to], dst.at[x], ssem.at[k], rsem.at[k],
                device_id=(g, e, to), device_id_type=MESH,
            ).start()

    def send_e(src, dst, k):
        for i in range(1, ne):
            to = lax.rem(e + i, ne)
            pltpu.make_async_remote_copy(
                src.at[to], dst.at[e], ssem.at[k], rsem.at[k],
                device_id=(g, to, x), device_id_type=MESH,
            ).start()

    def arrive(src, dst, k):
        n = dst.shape[0] - 1
        pltpu.make_async_copy(src.at[pl.ds(0, n)], dst.at[pl.ds(0, n)], ssem.at[k]).wait()
        pltpu.make_async_copy(src.at[pl.ds(0, n)], dst.at[pl.ds(0, n)], rsem.at[k]).wait()

    def scatter(cols):
        put(s0, cols, dot(pick0, normed[:, cols]))
        put(s1, cols, dot(pick1, normed[:, cols]))

    over_columns(scatter)
    pl.semaphore_wait(barrier, nx + ne - 2)
    send_x(s0, r0, 0)
    send_e(s1, r1, 1)
    r0[x] = s0[x]
    r1[e] = s1[e]
    arrive(s0, r0, 0)
    over_columns(lambda cols: put(t0, cols, dot(to_ex, get(r0, cols))))
    send_e(t0, q0, 2)
    q0[e] = t0[e]
    arrive(s1, r1, 1)
    over_columns(lambda cols: put(t1, cols, dot(to_xe, get(r1, cols))))
    send_x(t1, q1, 3)
    q1[x] = t1[x]

    for load in loads:
        load.wait()
    arrive(t0, q0, 2)
    arrive(t1, q1, 3)

    def collect(cols):
        xin[pl.ds(0, half), cols] = get(q0, cols)
        xin[pl.ds(half, half), cols] = get(q1, cols)

    over_columns(collect)
    ftile = 256

    def inner(i, carry):
        cols = pl.ds(pl.multiple_of(i * ftile, ftile), ftile)
        gate_proj = dot(xin[...], gate[:, cols])
        up_proj = dot(xin[...], up[:, cols])
        hid[:, cols] = (jax.nn.silu(gate_proj) * up_proj).astype(BF16)
        return carry

    lax.fori_loop(0, ff // ftile, inner, 0)

    def outer(cols):
        put(o0, cols, dot(hid[pl.ds(0, half), :], down[:, cols]))
        put(o1, cols, dot(hid[pl.ds(half, half), :], down[:, cols]))

    over_columns(outer)
    send_e(o0, b0, 4)
    send_x(o1, b1, 5)
    b0[e] = o0[e]
    b1[x] = o1[x]
    arrive(o0, b0, 4)
    over_columns(lambda cols: put(c0, cols, dot(to_xe, get(b0, cols))))
    send_x(c0, f0, 6)
    f0[x] = c0[x]
    arrive(o1, b1, 5)
    over_columns(lambda cols: put(c1, cols, dot(to_ex, get(b1, cols))))
    send_e(c1, f1, 7)
    f1[e] = c1[e]
    arrive(c0, f0, 6)
    arrive(c1, f1, 7)

    def combine(cols):
        moe = dot_t(pick0, get(f0, cols)) + dot_t(pick1, get(f1, cols))
        out_ref[:, cols] = (mixed_ref[:, cols].astype(F32) + moe).astype(BF16)

    over_columns(combine)


def moe(mixed, gain, row, col, gate_weight, up_weight, down_weight):
    nx, ne = lax.axis_size("rep"), lax.axis_size("ep")
    rows, width = mixed.shape
    ff = gate_weight.shape[2]
    half = nx * ne
    xe = pltpu.VMEM((nx, ne, width), BF16)
    ex = pltpu.VMEM((ne, nx, width), BF16)
    vmem, any_ = pl.BlockSpec(memory_space=pltpu.VMEM), pl.BlockSpec(memory_space=pl.ANY)
    return pl.pallas_call(
        functools.partial(moe_kernel, nx, ne),
        out_shape=jax.ShapeDtypeStruct((rows, width), BF16),
        in_specs=[vmem] * 4 + [any_] * 3,
        out_specs=vmem,
        scratch_shapes=[
            pltpu.VMEM((width, ff), BF16), pltpu.VMEM((width, ff), BF16), pltpu.VMEM((ff, width), BF16),
            pltpu.VMEM((rows, width), BF16), pltpu.VMEM((2 * half, width), BF16), pltpu.VMEM((2 * half, ff), BF16),
            xe, ex, xe, ex, ex, xe, ex, xe, ex, xe, ex, xe, xe, ex, xe, ex,
            pltpu.SemaphoreType.DMA((3,)), pltpu.SemaphoreType.DMA((8,)), pltpu.SemaphoreType.DMA((8,)),
        ],
        compiler_params=pltpu.CompilerParams(
            collective_id=1, has_side_effects=True, vmem_limit_bytes=48 << 20
        ),
        name="moe",
    )(
        mixed, gain.reshape(1, width), row, col,
        gate_weight[0], up_weight[0], down_weight[0],
    )


SHARED_ROWS = 1280


def front_kernel(
    nx, ne, prompt_ref, hidden_ref, query_ref, gain_ref, lengths_ref, ids_ref, idcol_ref,
    kvw_hbm, ow_hbm, table_hbm, mixed_ref, col_ref, row_ref,
    kvw, ow, table, picked, hn, pn, qf, qt, skv, dkv, spk, pkv, pf, kp, vp, att, full,
    lsem, ring_send, ring_recv, dd_send, dd_recv, xs, xr,
):
    e, x, g = lax.axis_index("ep"), lax.axis_index("rep"), lax.axis_index("groups")
    ny = ne // 2
    y, c = e // 2, lax.rem(e, 2)
    rows, width = hidden_ref.shape
    shared = SHARED_ROWS
    piece = shared // ne
    sub = (width - shared) // 4
    orow = ow.shape[1] // ne
    half = ow.shape[2] // 2
    plen = prompt_ref.shape[0] // GROUP_PROMPTS
    own_prompt = e // (ne // GROUP_PROMPTS)
    seqs = 16

    def sub_rows(core, s):
        start = pl.multiple_of(shared + core * (2 * sub) + s * sub, 16)
        return pl.ds(start, sub)

    def piece_rows(k, size, unit):
        return pl.ds(pl.multiple_of(k * unit, 16), size)

    loads = [
        pltpu.make_async_copy(
            kvw_hbm.at[pl.ds(shared, width - shared)], kvw.at[x, pl.ds(shared, width - shared)], lsem.at[0]
        ),
        pltpu.make_async_copy(
            kvw_hbm.at[piece_rows(e, piece, piece)], kvw.at[x, piece_rows(e, piece, piece)], lsem.at[1]
        ),
        pltpu.make_async_copy(
            ow_hbm.at[piece_rows(e, orow, orow)], ow.at[x, piece_rows(e, orow, orow)], lsem.at[2]
        ),
        pltpu.make_async_copy(table_hbm, table, lsem.at[3]),
    ]
    for load in loads:
        load.start()

    sibling = (g, 2 * y + 1 - c, x)

    def at_x(k):
        return (g, e, lax.rem(x + k + nx, nx))

    def at_y(k):
        return (g, 2 * lax.rem(y + k + ny, ny) + c, x)

    barrier = pltpu.get_barrier_semaphore()
    for i in range(1, nx):
        pl.semaphore_signal(barrier, inc=1, device_id=at_x(i), device_id_type=MESH)
    for i in range(1, ny):
        pl.semaphore_signal(barrier, inc=1, device_id=at_y(i), device_id_type=MESH)
    pl.semaphore_signal(barrier, inc=1, device_id=sibling, device_id_type=MESH)

    class Ring:
        def __init__(self, number, along, sign, hops, chunk, total, mate):
            self.along, self.sign, self.hops, self.chunk = along, sign, hops, chunk
            self.number, self.total, self.mate = number, total, mate

        def origin(self, h):
            me, n = (x, nx) if self.along == "x" else (y, ny)
            return lax.rem(me - self.sign * h + n, n)

        def go(self, h):
            ref = self.chunk(self.origin(h))
            to = at_x(self.sign) if self.along == "x" else at_y(self.sign)
            pltpu.make_async_remote_copy(
                ref, ref, ring_send.at[self.number], ring_recv.at[self.number, h],
                device_id=to, device_id_type=MESH,
            ).start()

        def event(self, h):
            if h > self.hops:
                return
            ref = self.chunk(self.origin(h))
            pltpu.make_async_copy(ref, ref, ring_recv.at[self.number, h - 1]).wait()
            if h < self.hops:
                self.go(h)
            if self.mate is not None:
                to_mate(ref, self.mate)

        def finish(self):
            ref = self.total(self.hops)
            pltpu.make_async_copy(ref, ref, ring_send.at[self.number]).wait()

    def to_mate(ref, k):
        pltpu.make_async_remote_copy(
            ref, ref, dd_send.at[k], dd_recv.at[k], device_id=sibling, device_id_type=MESH
        ).start()

    def mate_done(ref, k):
        pltpu.make_async_copy(ref, ref, dd_send.at[k]).wait()
        pltpu.make_async_copy(ref, ref, dd_recv.at[k]).wait()

    def rings(base, along, chunk, total, mate):
        made = []
        for s in range(2):
            for sign in (1, -1):
                hops = 4 if (s == 0) == (sign == 1) else 3
                made.append(
                    Ring(
                        base + len(made), along, sign, hops,
                        functools.partial(chunk, s), functools.partial(total, s), mate,
                    )
                )
        return made

    kv_x = rings(
        0, "x",
        lambda s, k: kvw.at[k, sub_rows(c, s)],
        lambda s, n: kvw.at[pl.ds(0, n), sub_rows(0, s)],
        0,
    )
    kv_y = rings(
        4, "y",
        lambda s, k: kvw.at[pl.ds(4 * s, 4), piece_rows(2 * k + c, piece, piece)],
        lambda s, n: kvw.at[pl.ds(4 * s, 4), pl.ds(0, n * piece)],
        1,
    )
    ow_x = rings(
        8, "x",
        lambda s, k: ow.at[k, piece_rows(e, orow, orow), pl.ds(s * half, half)],
        lambda s, n: ow.at[pl.ds(0, n), pl.ds(0, orow), pl.ds(s * half, half)],
        None,
    )
    ow_y = rings(
        12, "y",
        lambda s, k: ow.at[pl.ds(4 * s, 4), piece_rows(2 * k + c, orow, orow)],
        lambda s, n: ow.at[pl.ds(4 * s, 4), pl.ds(0, n * orow)],
        2,
    )

    def normalised(ref, out):
        widened = ref[...].astype(F32)
        scale = lax.rsqrt(jnp.mean(widened * widened, axis=-1, keepdims=True) + EPS)
        out[...] = (widened * scale * gain_ref[...]).astype(BF16)

    for load in loads:
        load.wait()
    pl.semaphore_wait(barrier, nx + ny - 1)

    own_piece = piece_rows(e, piece, piece)
    for i in range(1, nx):
        ref = kvw.at[x, own_piece]
        pltpu.make_async_remote_copy(
            ref, ref, xs.at[0], xr.at[0], device_id=at_x(i), device_id_type=MESH
        ).start()
    for ring in kv_x:
        ring.go(0)
    for ring in ow_x:
        ring.go(0)
    normalised(hidden_ref, hn)
    ref = kvw.at[pl.ds(0, nx - 1), pl.ds(0, piece)]
    pltpu.make_async_copy(ref, ref, xs.at[0]).wait()
    pltpu.make_async_copy(ref, ref, xr.at[0]).wait()
    for ring in kv_y:
        ring.go(0)
    for s in range(2):
        to_mate(kvw.at[pl.ds(4 * s, 4), own_piece], 1)

    for h in range(1, 5):
        for ring in kv_x:
            ring.event(h)
        for ring in kv_y:
            ring.event(h)
        for ring in ow_x:
            ring.event(h)
        if h == 1:
            normalised(prompt_ref, pn)
            for k in range(2):
                qf[k] = query_ref[:, pl.ds(k * HEAD_DIM, HEAD_DIM)].astype(F32)
        if h == 2:
            for t in range(nx):
                for k in range(2):
                    cols = pl.ds(k * HEAD_DIM, HEAD_DIM)
                    qt[t, :, cols] = qf[k, pl.ds(t, rows, stride=nx), :].astype(BF16)
        if h == 3:
            def look(i, carry):
                at = lax.div(ids_ref[i], 128)
                picked[pl.ds(i, 1), :] = table[pl.ds(at, 1), :]
                return carry

            lax.fori_loop(0, rows, look, 0)
            lane = lax.broadcasted_iota(jnp.int32, (rows, 128), 1)
            line = lax.broadcasted_iota(jnp.int32, (rows, 128), 0)
            chosen = jnp.sum(
                jnp.where(lane == lax.rem(idcol_ref[...], 128), picked[...], 0), axis=1, keepdims=True
            )
            col_ref[...] = chosen
            row_ref[...] = jnp.sum(jnp.where(lane == line, chosen, 0), axis=0, keepdims=True)
    mate_done(kvw.at[pl.ds(0, nx - 1), pl.ds(0, 2 * sub)], 0)
    mate_done(kvw.at[pl.ds(0, nx), pl.ds(0, ny * piece)], 1)

    length = lengths_ref[own_prompt]
    half_dim = HEAD_DIM // 2

    def turns(count, positions):
        lane = lax.broadcasted_iota(jnp.int32, (count, HEAD_DIM), 1)
        freq = jnp.exp(lax.rem(lane, half_dim).astype(F32) * (-2.0 * math.log(THETA) / HEAD_DIM))
        angles = positions.astype(F32) * freq
        sine = jnp.sin(angles)
        return jnp.cos(angles), jnp.where(lane < half_dim, -sine, sine)

    def turned(keys, cosine, sine):
        return keys * cosine + pltpu.roll(keys, half_dim, 1) * sine

    cosine, sine = turns(8, jnp.full((8, HEAD_DIM), length + x, jnp.int32))
    cosine, sine = cosine[0:1], sine[0:1]
    for head in range(KEY_VALUE_HEADS):
        skv[head, 0] = turned(dot(hn[...], kvw[2 * head]), cosine, sine).astype(BF16)
        skv[head, 1] = dot(hn[...], kvw[2 * head + 1]).astype(BF16)
    for i in range(1, nx):
        to = lax.rem(x + i, nx)
        pltpu.make_async_remote_copy(
            skv.at[to // 2], dkv.at[x], xs.at[1], xr.at[1], device_id=(g, e, to), device_id_type=MESH
        ).start()
    dkv[x] = skv[x // 2]

    count = GROUP_PROMPTS * plen
    line = lax.broadcasted_iota(jnp.int32, (count, HEAD_DIM), 0)
    pcos, psin = turns(count, e * plen + lax.rem(line, plen))
    head = x // 2
    pkey = turned(dot(pn[...], kvw[2 * head]), pcos, psin)
    pval = dot(pn[...], kvw[2 * head + 1])
    spk[:, 0] = pkey.reshape(GROUP_PROMPTS, plen, HEAD_DIM).astype(BF16)
    spk[:, 1] = pval.reshape(GROUP_PROMPTS, plen, HEAD_DIM).astype(BF16)
    per = ny // GROUP_PROMPTS
    for i in range(1, ny):
        to = lax.rem(y + i, ny)
        pltpu.make_async_remote_copy(
            spk.at[to // per], pkv.at[c, y], xs.at[2], xr.at[2],
            device_id=(g, 2 * to + c, x), device_id_type=MESH,
        ).start()
    pkv[c, y] = spk[y // per]
    for ring in ow_y:
        ring.go(0)
    for s in range(2):
        to_mate(ow.at[pl.ds(4 * s, 4), piece_rows(e, orow, orow)], 2)

    ref = pkv.at[0, pl.ds(0, ny - 1)]
    pltpu.make_async_copy(ref, ref, xs.at[2]).wait()
    pltpu.make_async_copy(ref, ref, xr.at[2]).wait()
    to_mate(pkv.at[c], 3)
    mate_done(pkv.at[0], 3)
    for k in range(2):
        for core in range(2):
            for row in range(ny):
                start = (2 * row + core) * plen
                pf[pl.ds(start, plen), :] = pkv[core, row, k].astype(F32)
        (kp if k == 0 else vp)[...] = pf[...].astype(BF16)

    for ring in ow_y:
        ring.event(1)

    ref = dkv.at[pl.ds(0, nx - 1)]
    pltpu.make_async_copy(ref, ref, xs.at[1]).wait()
    pltpu.make_async_copy(ref, ref, xr.at[1]).wait()

    keys = kp.shape[0]
    block = 2 * nx * seqs
    scale = HEAD_DIM ** (-0.5)
    valid = lax.broadcasted_iota(jnp.int32, (block, keys), 1) < length
    r = lax.rem(lax.broadcasted_iota(jnp.int32, (block, nx * seqs), 0), nx * seqs)
    k = lax.broadcasted_iota(jnp.int32, (block, nx * seqs), 1)
    own = (lax.rem(r, seqs) == lax.rem(k, seqs)) & (k // seqs <= r // seqs)

    def nt(a, b):
        return lax.dot_general(a, b, (((1,), (1,)), ((), ())), preferred_element_type=F32)

    def attend(j, carry):
        pick = pl.ds(pl.multiple_of(j * seqs, seqs), seqs)
        q2 = jnp.concatenate(
            [qt[:, pick, pl.ds(h * HEAD_DIM, HEAD_DIM)].reshape(nx * seqs, HEAD_DIM) for h in range(2)], axis=0
        )
        sp = jnp.where(valid, nt(q2, kp[...]) * scale, -1e30)
        sd = jnp.where(own, nt(q2, dkv[:, 0, pick].reshape(nx * seqs, HEAD_DIM)) * scale, -1e30)
        top = jnp.maximum(jnp.max(sp, axis=1, keepdims=True), jnp.max(sd, axis=1, keepdims=True))
        wp = jnp.where(valid, jnp.exp(sp - top), 0.0)
        wd = jnp.where(own, jnp.exp(sd - top), 0.0)
        total = jnp.sum(wp, axis=1, keepdims=True) + jnp.sum(wd, axis=1, keepdims=True)
        summed = dot(wp.astype(BF16), vp[...])
        summed = summed + dot(wd.astype(BF16), dkv[:, 1, pick].reshape(nx * seqs, HEAD_DIM))
        result = (summed / total).astype(BF16)
        for h in range(2):
            att[:, pick, pl.ds(h * HEAD_DIM, HEAD_DIM)] = result[h * nx * seqs:(h + 1) * nx * seqs].reshape(
                nx, seqs, HEAD_DIM
            )
        return carry

    lax.fori_loop(0, rows // seqs, attend, 0)
    for i in range(1, nx):
        to = lax.rem(x + i, nx)
        pltpu.make_async_remote_copy(
            att.at[to], full.at[x], xs.at[3], xr.at[3], device_id=(g, e, to), device_id_type=MESH
        ).start()
    full[x] = att[x]
    for h in range(2, 5):
        for ring in ow_y:
            ring.event(h)
    ref = full.at[pl.ds(0, nx - 1)]
    pltpu.make_async_copy(ref, ref, xs.at[3]).wait()
    pltpu.make_async_copy(ref, ref, xr.at[3]).wait()
    mate_done(ow.at[pl.ds(0, nx), pl.ds(0, ny * orow)], 2)

    tile = 512

    def project(i, carry):
        cols = pl.ds(pl.multiple_of(i * tile, tile), tile)
        total = dot(full[0], ow[0, :, cols])
        for k in range(1, nx):
            total = total + dot(full[k], ow[k, :, cols])
        mixed_ref[:, cols] = (hidden_ref[:, cols].astype(F32) + total).astype(BF16)
        return carry

    lax.fori_loop(0, width // tile, project, 0)
    for ring in kv_x + kv_y + ow_x + ow_y:
        ring.finish()


def front(prompt, hidden, queries, gain, lengths, ids, kvw, ow, expert_table):
    nx, ne = lax.axis_size("rep"), lax.axis_size("ep")
    rows, width = hidden.shape
    count = prompt.shape[0]
    plen = count // GROUP_PROMPTS
    keys = plen * ne
    vmem, any_ = pl.BlockSpec(memory_space=pltpu.VMEM), pl.BlockSpec(memory_space=pl.ANY)
    smem = pl.BlockSpec(memory_space=pltpu.SMEM)
    cols = queries.shape[1]
    table = expert_table.reshape(-1, 128)
    sem = pltpu.SemaphoreType.DMA
    return pl.pallas_call(
        functools.partial(front_kernel, nx, ne),
        out_shape=(
            jax.ShapeDtypeStruct((rows, width), BF16),
            jax.ShapeDtypeStruct((rows, 1), jnp.int32),
            jax.ShapeDtypeStruct((1, rows), jnp.int32),
        ),
        in_specs=[vmem] * 4 + [smem] * 2 + [vmem] + [any_] * 3,
        out_specs=(vmem, vmem, vmem),
        scratch_shapes=[
            pltpu.VMEM((nx,) + kvw.shape, BF16),
            pltpu.VMEM((nx,) + ow.shape, BF16),
            pltpu.VMEM(table.shape, jnp.int32),
            pltpu.VMEM((rows, 128), jnp.int32),
            pltpu.VMEM((rows, width), BF16),
            pltpu.VMEM((count, width), BF16),
            pltpu.VMEM((2, queries.shape[0], HEAD_DIM), F32),
            pltpu.VMEM((nx, rows, cols), BF16),
            pltpu.VMEM((KEY_VALUE_HEADS, 2, rows, HEAD_DIM), BF16),
            pltpu.VMEM((nx, 2, rows, HEAD_DIM), BF16),
            pltpu.VMEM((GROUP_PROMPTS, 2, plen, HEAD_DIM), BF16),
            pltpu.VMEM((2, ne // 2, 2, plen, HEAD_DIM), BF16),
            pltpu.VMEM((keys, HEAD_DIM), F32),
            pltpu.VMEM((keys, HEAD_DIM), BF16),
            pltpu.VMEM((keys, HEAD_DIM), BF16),
            pltpu.VMEM((nx, rows, cols), BF16),
            pltpu.VMEM((nx, rows, cols), BF16),
            sem((4,)), sem((16,)), sem((16, 4)), sem((4,)), sem((4,)), sem((4,)), sem((4,)),
        ],
        compiler_params=pltpu.CompilerParams(
            collective_id=0, has_side_effects=True, vmem_limit_bytes=48 << 20
        ),
        name="front",
    )(
        prompt, hidden, queries, gain.reshape(1, width), lengths, ids.reshape(rows), ids.reshape(rows, 1),
        kvw, ow, table,
    )


def local(
    prompt_hidden,
    decode_hidden,
    queries,
    attn_gain,
    key_value_weight,
    out_weight,
    moe_gain,
    gate_weight,
    up_weight,
    down_weight,
    expert_table,
    token_ids,
    prompt_lengths,
):
    rows = decode_hidden.shape[0] * decode_hidden.shape[1]
    width = decode_hidden.shape[2]
    mixed, col, row = front(
        prompt_hidden.reshape(-1, width),
        decode_hidden.reshape(rows, width),
        queries.reshape(-1, queries.shape[2]),
        attn_gain,
        prompt_lengths,
        token_ids,
        key_value_weight,
        out_weight,
        expert_table,
    )
    out = moe(mixed, moe_gain, row, col, gate_weight, up_weight, down_weight)
    return out.reshape(decode_hidden.shape)


def solution(mesh):
    placed = (
        P("groups", "ep", None),
        P(("groups", "ep"), "rep", None),
        P(("groups", "ep"), None, "rep"),
        P(),
        P(None, "rep"),
        P("rep", None),
        P(),
        P(("ep", "rep"), None, None),
        P(("ep", "rep"), None, None),
        P(("ep", "rep"), None, None),
        P(),
        P("ep", "rep"),
        P("groups"),
    )
    return jax.shard_map(
        local,
        mesh=mesh,
        in_specs=placed,
        out_specs=P(("groups", "ep"), "rep", None),
        check_vma=False,
    )
```

```python
import functools
import math

import jax
import jax.numpy as jnp
from jax import lax
from jax.experimental import pallas as pl
from jax.experimental.pallas import tpu as pltpu
from jax.sharding import PartitionSpec as P

HEAD_DIM = 128
QUERY_HEADS = 16
KEY_VALUE_HEADS = 4
GROUP_PROMPTS = 4
CAP = 2

EPS = 1e-06
THETA = 1000000.0
MESH = pl.DeviceIdType.MESH
F32 = jnp.float32
BF16 = jnp.bfloat16


def dot(a, b):
    return jnp.dot(a, b, preferred_element_type=F32)


def dot_t(a, b):
    return lax.dot_general(a, b, (((0,), (0,)), ((), ())), preferred_element_type=F32)


def one_hot(hit):
    return jnp.where(hit, 1.0, 0.0).astype(BF16)


SHARED_ROWS = 1280
CHUNKS = 2


def layer_kernel(
    nx, ne, prompt_hbm, hidden_hbm, query_hbm, gain_ref, moe_gain_ref, lengths_ref, ids_ref, idrow_ref,
    kvw_hbm, ow_hbm, table_hbm, gate_hbm, up_hbm, down_hbm, out_ref,
    prompt_ref, hidden_ref, query_ref,
    kvw, ow, table, picked, hn, pn, qf, qt, skv, dkv, spk, pkv, pf, kp, vp, att, full, mixed_ref,
    gate, up, down, normed, hid, gate_acc, up_acc,
    s0, s1, r0, r1, t0, t1, q0, q1, o0, o1, b0, b1, c0, c1, f0, f1,
    lsem, wsem, ring_send, ring_recv, dd_send, dd_recv, xs, xr, msend, mrecv,
):
    e, x, g = lax.axis_index("ep"), lax.axis_index("rep"), lax.axis_index("groups")
    ny = ne // 2
    y, c = e // 2, lax.rem(e, 2)
    rows, width = hidden_hbm.shape
    shared = SHARED_ROWS
    piece = shared // ne
    sub = (width - shared) // 4
    orow = ow.shape[1] // ne
    half = ow.shape[2] // 2
    plen = prompt_hbm.shape[0] // GROUP_PROMPTS
    own_prompt = e // (ne // GROUP_PROMPTS)
    seqs = 16

    def sub_rows(core, s):
        start = pl.multiple_of(shared + core * (2 * sub) + s * sub, 16)
        return pl.ds(start, sub)

    def piece_rows(k, size, unit):
        return pl.ds(pl.multiple_of(k * unit, 16), size)

    loads = [
        pltpu.make_async_copy(
            kvw_hbm.at[pl.ds(shared, width - shared)], kvw.at[x, pl.ds(shared, width - shared)], lsem.at[0]
        ),
        pltpu.make_async_copy(
            kvw_hbm.at[piece_rows(e, piece, piece)], kvw.at[x, piece_rows(e, piece, piece)], lsem.at[1]
        ),
        pltpu.make_async_copy(
            ow_hbm.at[piece_rows(e, orow, orow)], ow.at[x, piece_rows(e, orow, orow)], lsem.at[2]
        ),
    ]
    late = [
        pltpu.make_async_copy(hidden_hbm, hidden_ref, lsem.at[3]),
        pltpu.make_async_copy(prompt_hbm, prompt_ref, lsem.at[4]),
        pltpu.make_async_copy(query_hbm, query_ref, lsem.at[5]),
        pltpu.make_async_copy(table_hbm, table, lsem.at[6]),
    ]
    weights = [
        pltpu.make_async_copy(gate_hbm, gate, wsem.at[0]),
        pltpu.make_async_copy(up_hbm, up, wsem.at[1]),
        pltpu.make_async_copy(down_hbm, down, wsem.at[2]),
    ]
    for load in loads + late:
        load.start()

    sibling = (g, 2 * y + 1 - c, x)

    def at_x(k):
        return (g, e, lax.rem(x + k + nx, nx))

    def at_y(k):
        return (g, 2 * lax.rem(y + k + ny, ny) + c, x)

    barrier = pltpu.get_barrier_semaphore()
    for i in range(1, nx):
        pl.semaphore_signal(barrier, inc=1, device_id=at_x(i), device_id_type=MESH)
    for i in range(1, ne):
        peer = (g, lax.rem(e + i, ne), x)
        pl.semaphore_signal(barrier, inc=1, device_id=peer, device_id_type=MESH)

    class Ring:
        def __init__(self, number, along, sign, hops, chunk, total, mate):
            self.along, self.sign, self.hops, self.chunk = along, sign, hops, chunk
            self.number, self.total, self.mate = number, total, mate

        def origin(self, h):
            me, n = (x, nx) if self.along == "x" else (y, ny)
            return lax.rem(me - self.sign * h + n, n)

        def go(self, h):
            ref = self.chunk(self.origin(h))
            to = at_x(self.sign) if self.along == "x" else at_y(self.sign)
            pltpu.make_async_remote_copy(
                ref, ref, ring_send.at[self.number], ring_recv.at[self.number, h],
                device_id=to, device_id_type=MESH,
            ).start()

        def event(self, h):
            if h > self.hops:
                return
            ref = self.chunk(self.origin(h))
            pltpu.make_async_copy(ref, ref, ring_recv.at[self.number, h - 1]).wait()
            if h < self.hops:
                self.go(h)
            if self.mate is not None:
                to_mate(ref, self.mate)

        def finish(self):
            ref = self.total(self.hops)
            pltpu.make_async_copy(ref, ref, ring_send.at[self.number]).wait()

    def to_mate(ref, k):
        pltpu.make_async_remote_copy(
            ref, ref, dd_send.at[k], dd_recv.at[k], device_id=sibling, device_id_type=MESH
        ).start()

    def mate_done(ref, k):
        pltpu.make_async_copy(ref, ref, dd_send.at[k]).wait()
        pltpu.make_async_copy(ref, ref, dd_recv.at[k]).wait()

    def rings(base, along, chunk, total, mate):
        made = []
        for s in range(2):
            for sign in (1, -1):
                hops = 4 if (s == 0) == (sign == 1) else 3
                made.append(
                    Ring(
                        base + len(made), along, sign, hops,
                        functools.partial(chunk, s), functools.partial(total, s), mate,
                    )
                )
        return made

    kv_x = rings(
        0, "x",
        lambda s, k: kvw.at[k, sub_rows(c, s)],
        lambda s, n: kvw.at[pl.ds(0, n), sub_rows(0, s)],
        0,
    )
    kv_y = rings(
        4, "y",
        lambda s, k: kvw.at[pl.ds(4 * s, 4), piece_rows(2 * k + c, piece, piece)],
        lambda s, n: kvw.at[pl.ds(4 * s, 4), pl.ds(0, n * piece)],
        1,
    )
    ow_x = rings(
        8, "x",
        lambda s, k: ow.at[k, piece_rows(e, orow, orow), pl.ds(s * half, half)],
        lambda s, n: ow.at[pl.ds(0, n), pl.ds(0, orow), pl.ds(s * half, half)],
        None,
    )
    ow_y = rings(
        12, "y",
        lambda s, k: ow.at[pl.ds(4 * s, 4), piece_rows(2 * k + c, orow, orow)],
        lambda s, n: ow.at[pl.ds(4 * s, 4), pl.ds(0, n * orow)],
        2,
    )

    def normalised(ref, out):
        widened = ref[...].astype(F32)
        scale = lax.rsqrt(jnp.mean(widened * widened, axis=-1, keepdims=True) + EPS)
        out[...] = (widened * scale * gain_ref[...]).astype(BF16)

    with jax.named_scope("enter"):
        for load in loads:
            load.wait()
        pl.semaphore_wait(barrier, nx + ne - 2)

    own_piece = piece_rows(e, piece, piece)
    for i in range(1, nx):
        ref = kvw.at[x, own_piece]
        pltpu.make_async_remote_copy(
            ref, ref, xs.at[0], xr.at[0], device_id=at_x(i), device_id_type=MESH
        ).start()
    for ring in kv_x:
        ring.go(0)
    for ring in ow_x:
        ring.go(0)
    for load in late:
        load.wait()
    normalised(hidden_ref, hn)
    ref = kvw.at[pl.ds(0, nx - 1), pl.ds(0, piece)]
    pltpu.make_async_copy(ref, ref, xs.at[0]).wait()
    pltpu.make_async_copy(ref, ref, xr.at[0]).wait()
    for ring in kv_y:
        ring.go(0)
    for s in range(2):
        to_mate(kvw.at[pl.ds(4 * s, 4), own_piece], 1)

    for h in range(1, 5):
        with jax.named_scope("kv_x"):
            for ring in kv_x:
                ring.event(h)
        with jax.named_scope("kv_y"):
            for ring in kv_y:
                ring.event(h)
        with jax.named_scope("ow_x"):
            for ring in ow_x:
                ring.event(h)
        if h == 1:
            normalised(prompt_ref, pn)
            for k in range(2):
                qf[k] = query_ref[:, pl.ds(k * HEAD_DIM, HEAD_DIM)].astype(F32)
        if h == 2:
            for t in range(nx):
                for k in range(2):
                    cols = pl.ds(k * HEAD_DIM, HEAD_DIM)
                    qt[t, :, cols] = qf[k, pl.ds(t, rows, stride=nx), :].astype(BF16)
        if h == 3:
            def look(i, carry):
                at = lax.div(ids_ref[i], 128)
                picked[pl.ds(i, 1), :] = table[pl.ds(at, 1), :]
                return carry

            lax.fori_loop(0, rows, look, 0)
            for weight in weights:
                weight.start()
    mate_done(kvw.at[pl.ds(0, nx - 1), pl.ds(0, 2 * sub)], 0)
    mate_done(kvw.at[pl.ds(0, nx), pl.ds(0, ny * piece)], 1)

    length = lengths_ref[own_prompt]
    half_dim = HEAD_DIM // 2

    def turns(count, positions):
        lane = lax.broadcasted_iota(jnp.int32, (count, HEAD_DIM), 1)
        freq = jnp.exp(lax.rem(lane, half_dim).astype(F32) * (-2.0 * math.log(THETA) / HEAD_DIM))
        angles = positions.astype(F32) * freq
        sine = jnp.sin(angles)
        return jnp.cos(angles), jnp.where(lane < half_dim, -sine, sine)

    def turned(keys, cosine, sine):
        return keys * cosine + pltpu.roll(keys, half_dim, 1) * sine

    cosine, sine = turns(8, jnp.full((8, HEAD_DIM), length + x, jnp.int32))
    cosine, sine = cosine[0:1], sine[0:1]
    for head in range(KEY_VALUE_HEADS):
        skv[head, 0] = turned(dot(hn[...], kvw[2 * head]), cosine, sine).astype(BF16)
        skv[head, 1] = dot(hn[...], kvw[2 * head + 1]).astype(BF16)
    for i in range(1, nx):
        to = lax.rem(x + i, nx)
        pltpu.make_async_remote_copy(
            skv.at[to // 2], dkv.at[x], xs.at[1], xr.at[1], device_id=(g, e, to), device_id_type=MESH
        ).start()
    dkv[x] = skv[x // 2]

    count = GROUP_PROMPTS * plen
    line = lax.broadcasted_iota(jnp.int32, (count, HEAD_DIM), 0)
    pcos, psin = turns(count, e * plen + lax.rem(line, plen))
    head = x // 2
    pkey = turned(dot(pn[...], kvw[2 * head]), pcos, psin)
    pval = dot(pn[...], kvw[2 * head + 1])
    spk[:, 0] = pkey.reshape(GROUP_PROMPTS, plen, HEAD_DIM).astype(BF16)
    spk[:, 1] = pval.reshape(GROUP_PROMPTS, plen, HEAD_DIM).astype(BF16)
    per = ny // GROUP_PROMPTS
    for i in range(1, ny):
        to = lax.rem(y + i, ny)
        pltpu.make_async_remote_copy(
            spk.at[to // per], pkv.at[c, y], xs.at[2], xr.at[2],
            device_id=(g, 2 * to + c, x), device_id_type=MESH,
        ).start()
    pkv[c, y] = spk[y // per]
    for ring in ow_y:
        ring.go(0)
    for s in range(2):
        to_mate(ow.at[pl.ds(4 * s, 4), piece_rows(e, orow, orow)], 2)

    ref = pkv.at[0, pl.ds(0, ny - 1)]
    pltpu.make_async_copy(ref, ref, xs.at[2]).wait()
    pltpu.make_async_copy(ref, ref, xr.at[2]).wait()
    to_mate(pkv.at[c], 3)
    mate_done(pkv.at[0], 3)
    for k in range(2):
        for core in range(2):
            for row in range(ny):
                start = (2 * row + core) * plen
                pf[pl.ds(start, plen), :] = pkv[core, row, k].astype(F32)
        (kp if k == 0 else vp)[...] = pf[...].astype(BF16)

    for ring in ow_y:
        ring.event(1)

    ref = dkv.at[pl.ds(0, nx - 1)]
    pltpu.make_async_copy(ref, ref, xs.at[1]).wait()
    pltpu.make_async_copy(ref, ref, xr.at[1]).wait()

    keys = kp.shape[0]
    block = 2 * nx * seqs
    scale = HEAD_DIM ** (-0.5)
    valid = lax.broadcasted_iota(jnp.int32, (block, keys), 1) < length
    r = lax.rem(lax.broadcasted_iota(jnp.int32, (block, nx * seqs), 0), nx * seqs)
    k = lax.broadcasted_iota(jnp.int32, (block, nx * seqs), 1)
    own = (lax.rem(r, seqs) == lax.rem(k, seqs)) & (k // seqs <= r // seqs)

    def nt(a, b):
        return lax.dot_general(a, b, (((1,), (1,)), ((), ())), preferred_element_type=F32)

    def attend(j, carry):
        pick = pl.ds(pl.multiple_of(j * seqs, seqs), seqs)
        q2 = jnp.concatenate(
            [qt[:, pick, pl.ds(h * HEAD_DIM, HEAD_DIM)].reshape(nx * seqs, HEAD_DIM) for h in range(2)], axis=0
        )
        sp = jnp.where(valid, nt(q2, kp[...]) * scale, -1e30)
        sd = jnp.where(own, nt(q2, dkv[:, 0, pick].reshape(nx * seqs, HEAD_DIM)) * scale, -1e30)
        top = jnp.maximum(jnp.max(sp, axis=1, keepdims=True), jnp.max(sd, axis=1, keepdims=True))
        wp = jnp.where(valid, jnp.exp(sp - top), 0.0)
        wd = jnp.where(own, jnp.exp(sd - top), 0.0)
        total = jnp.sum(wp, axis=1, keepdims=True) + jnp.sum(wd, axis=1, keepdims=True)
        summed = dot(wp.astype(BF16), vp[...])
        summed = summed + dot(wd.astype(BF16), dkv[:, 1, pick].reshape(nx * seqs, HEAD_DIM))
        result = (summed / total).astype(BF16)
        for h in range(2):
            att[:, pick, pl.ds(h * HEAD_DIM, HEAD_DIM)] = result[h * nx * seqs:(h + 1) * nx * seqs].reshape(
                nx, seqs, HEAD_DIM
            )
        return carry

    lax.fori_loop(0, rows // seqs, attend, 0)
    for i in range(1, nx):
        to = lax.rem(x + i, nx)
        pltpu.make_async_remote_copy(
            att.at[to], full.at[x], xs.at[3], xr.at[3], device_id=(g, e, to), device_id_type=MESH
        ).start()
    full[x] = att[x]
    for h in range(2, 5):
        for ring in ow_y:
            ring.event(h)
    ref = full.at[pl.ds(0, nx - 1)]
    pltpu.make_async_copy(ref, ref, xs.at[3]).wait()
    pltpu.make_async_copy(ref, ref, xr.at[3]).wait()
    mate_done(ow.at[pl.ds(0, nx), pl.ds(0, ny * orow)], 2)

    tile = 512

    def project(i, carry):
        cols = pl.ds(pl.multiple_of(i * tile, tile), tile)
        total = dot(full[0], ow[0, :, cols])
        for k in range(1, nx):
            total = total + dot(full[k], ow[k, :, cols])
        mixed_ref[:, cols] = (hidden_ref[:, cols].astype(F32) + total).astype(BF16)
        return carry

    lax.fori_loop(0, width // tile, project, 0)
    lane = lax.broadcasted_iota(jnp.int32, (rows, rows), 1)
    line = lax.broadcasted_iota(jnp.int32, (rows, rows), 0)
    idcol = jnp.sum(jnp.where(lane == line, idrow_ref[...], 0), axis=1, keepdims=True)
    col = jnp.sum(jnp.where(lane == lax.rem(idcol, 128), picked[...], 0), axis=1, keepdims=True)
    row = jnp.sum(jnp.where(lane == line, col, 0), axis=0, keepdims=True)
    earlier = jnp.where((row == col) & (line < lane), 1, 0)
    rank = jnp.sum(earlier, axis=0, keepdims=True)
    cells = nx * ne
    slot = lax.broadcasted_iota(jnp.int32, (cells, rows), 0)
    swapped = lax.rem(slot, ne) * nx + slot // ne
    pick0 = one_hot((swapped == row) & (rank == 0))
    pick1 = one_hot((slot == row) & (rank == 1))
    here = lax.broadcasted_iota(jnp.int32, (cells, cells), 0)
    there = lax.broadcasted_iota(jnp.int32, (cells, cells), 1)
    to_ex = one_hot(there == lax.rem(here, nx) * ne + here // nx)
    to_xe = one_hot(there == lax.rem(here, ne) * nx + here // ne)

    with jax.named_scope("moe_norm"):
        widened = mixed_ref[...].astype(F32)
        scale = lax.rsqrt(jnp.mean(widened * widened, axis=-1, keepdims=True) + EPS)
        normed[...] = (widened * scale * moe_gain_ref[...]).astype(BF16)

    part = width // CHUNKS
    tile = 512

    def tiles(chunk, body):
        def step(i, carry):
            body(pl.ds(pl.multiple_of(chunk * part + i * tile, tile), tile))
            return carry

        lax.fori_loop(0, part // tile, step, 0)

    def put(ref, cols, value):
        ref[:, :, cols] = value.reshape(ref.shape[0], ref.shape[1], tile).astype(BF16)

    def get(ref, cols):
        return ref[:, :, cols].astype(F32).reshape(cells, tile).astype(BF16)

    def send(src, dst, k, chunk):
        n = dst.shape[0]
        me = x if n == nx else e
        cols = pl.ds(chunk * part, part)
        for i in range(1, n):
            to = lax.rem(me + i, n)
            pltpu.make_async_remote_copy(
                src.at[to, :, cols], dst.at[me, :, cols], msend.at[k, chunk], mrecv.at[k, chunk],
                device_id=(g, e, to) if n == nx else (g, to, x), device_id_type=MESH,
            ).start()
        dst[me, :, cols] = src[me, :, cols]

    def arrive(dst, k, chunk):
        ref = dst.at[pl.ds(0, dst.shape[0] - 1), :, pl.ds(chunk * part, part)]
        pltpu.make_async_copy(ref, ref, msend.at[k, chunk]).wait()
        pltpu.make_async_copy(ref, ref, mrecv.at[k, chunk]).wait()

    def two_phases(base, a0, m0, n0, d0, a1, m1, n1, d1, order0, order1, fill):
        for chunk in range(CHUNKS):
            with jax.named_scope("fill"):
                fill(chunk)
            send(a0, m0, base, chunk)
            send(a1, m1, base + 1, chunk)
        for chunk in range(CHUNKS):
            with jax.named_scope("wait_first"):
                arrive(m0, base, chunk)
            with jax.named_scope("permute"):
                tiles(chunk, lambda cols: put(n0, cols, dot(order0, get(m0, cols))))
            send(n0, d0, base + 2, chunk)
            with jax.named_scope("wait_first"):
                arrive(m1, base + 1, chunk)
            with jax.named_scope("permute"):
                tiles(chunk, lambda cols: put(n1, cols, dot(order1, get(m1, cols))))
            send(n1, d1, base + 3, chunk)

    def scatter(chunk):
        def body(cols):
            put(s0, cols, dot(pick0, normed[:, cols]))
            put(s1, cols, dot(pick1, normed[:, cols]))

        tiles(chunk, body)

    two_phases(0, s0, r0, t0, q0, s1, r1, t1, q1, to_ex, to_xe, scatter)
    with jax.named_scope("weights"):
        for weight in weights:
            weight.wait()

    ff = gate.shape[1]
    ftile = 256
    for chunk in range(CHUNKS):
        with jax.named_scope("wait_second"):
            arrive(q0, 2, chunk)
            arrive(q1, 3, chunk)
        with jax.named_scope("inner"):
            cols = pl.ds(chunk * part, part)
            tokens = jnp.concatenate(
                [q[:, :, cols].astype(F32).reshape(cells, part).astype(BF16) for q in (q0, q1)], axis=0
            )
            if chunk == 0:
                gate_acc[...] = dot(tokens, gate[cols, :])
                up_acc[...] = dot(tokens, up[cols, :])
            else:
                gate_acc[...] += dot(tokens, gate[cols, :])
                up_acc[...] += dot(tokens, up[cols, :])
    with jax.named_scope("silu"):
        hid[...] = (jax.nn.silu(gate_acc[...]) * up_acc[...]).astype(BF16)

    def outer(chunk):
        def body(cols):
            put(o0, cols, dot(hid[pl.ds(0, cells), :], down[:, cols]))
            put(o1, cols, dot(hid[pl.ds(cells, cells), :], down[:, cols]))

        tiles(chunk, body)

    two_phases(4, o0, b0, c0, f0, o1, b1, c1, f1, to_xe, to_ex, outer)
    for chunk in range(CHUNKS):
        with jax.named_scope("wait_second"):
            arrive(f0, 6, chunk)
            arrive(f1, 7, chunk)

        def combine(cols):
            moe = dot_t(pick0, get(f0, cols)) + dot_t(pick1, get(f1, cols))
            out_ref[:, cols] = (mixed_ref[:, cols].astype(F32) + moe).astype(BF16)

        with jax.named_scope("combine"):
            tiles(chunk, combine)
    for ring in kv_x + kv_y + ow_x + ow_y:
        ring.finish()


def layer(prompt, hidden, queries, gain, moe_gain, lengths, ids, kvw, ow, expert_table, gate, up, down):
    nx, ne = lax.axis_size("rep"), lax.axis_size("ep")
    rows, width = hidden.shape
    count = prompt.shape[0]
    plen = count // GROUP_PROMPTS
    keys = plen * ne
    ff = gate.shape[1]
    vmem, any_ = pl.BlockSpec(memory_space=pltpu.VMEM), pl.BlockSpec(memory_space=pl.ANY)
    smem = pl.BlockSpec(memory_space=pltpu.SMEM)
    cols = queries.shape[1]
    table = expert_table.reshape(-1, 128)
    sem = pltpu.SemaphoreType.DMA
    xe = pltpu.VMEM((nx, ne, width), BF16)
    ex = pltpu.VMEM((ne, nx, width), BF16)
    return pl.pallas_call(
        functools.partial(layer_kernel, nx, ne),
        out_shape=jax.ShapeDtypeStruct((rows, width), BF16),
        in_specs=[any_] * 3 + [vmem] * 2 + [smem] * 2 + [vmem] + [any_] * 6,
        out_specs=vmem,
        scratch_shapes=[
            pltpu.VMEM(prompt.shape, BF16),
            pltpu.VMEM(hidden.shape, BF16),
            pltpu.VMEM(queries.shape, BF16),
            pltpu.VMEM((nx,) + kvw.shape, BF16),
            pltpu.VMEM((nx,) + ow.shape, BF16),
            pltpu.VMEM(table.shape, jnp.int32),
            pltpu.VMEM((rows, 128), jnp.int32),
            pltpu.VMEM((rows, width), BF16),
            pltpu.VMEM((count, width), BF16),
            pltpu.VMEM((2, queries.shape[0], HEAD_DIM), F32),
            pltpu.VMEM((nx, rows, cols), BF16),
            pltpu.VMEM((KEY_VALUE_HEADS, 2, rows, HEAD_DIM), BF16),
            pltpu.VMEM((nx, 2, rows, HEAD_DIM), BF16),
            pltpu.VMEM((GROUP_PROMPTS, 2, plen, HEAD_DIM), BF16),
            pltpu.VMEM((2, ne // 2, 2, plen, HEAD_DIM), BF16),
            pltpu.VMEM((keys, HEAD_DIM), F32),
            pltpu.VMEM((keys, HEAD_DIM), BF16),
            pltpu.VMEM((keys, HEAD_DIM), BF16),
            pltpu.VMEM((nx, rows, cols), BF16),
            pltpu.VMEM((nx, rows, cols), BF16),
            pltpu.VMEM((rows, width), BF16),
            pltpu.VMEM(gate.shape, BF16), pltpu.VMEM(up.shape, BF16), pltpu.VMEM(down.shape, BF16),
            pltpu.VMEM((rows, width), BF16), pltpu.VMEM((2 * nx * ne, ff), BF16),
            pltpu.VMEM((2 * nx * ne, ff), F32), pltpu.VMEM((2 * nx * ne, ff), F32),
            xe, ex, xe, ex, ex, xe, ex, xe, ex, xe, ex, xe, xe, ex, xe, ex,
            sem((7,)), sem((3,)), sem((16,)), sem((16, 4)), sem((4,)), sem((4,)), sem((4,)), sem((4,)),
            sem((8, CHUNKS)), sem((8, CHUNKS)),
        ],
        compiler_params=pltpu.CompilerParams(
            collective_id=0, has_side_effects=True, vmem_limit_bytes=67043328
        ),
        name="layer",
    )(
        prompt, hidden, queries, gain.reshape(1, width), moe_gain.reshape(1, width), lengths,
        ids.reshape(rows), ids.reshape(1, rows), kvw, ow, table, gate, up, down,
    )


def local(
    prompt_hidden,
    decode_hidden,
    queries,
    attn_gain,
    key_value_weight,
    out_weight,
    moe_gain,
    gate_weight,
    up_weight,
    down_weight,
    expert_table,
    token_ids,
    prompt_lengths,
):
    width = decode_hidden.shape[2]
    out = layer(
        prompt_hidden.reshape(-1, width),
        decode_hidden.reshape(-1, width),
        queries.reshape(-1, queries.shape[2]),
        attn_gain,
        moe_gain,
        prompt_lengths,
        token_ids,
        key_value_weight,
        out_weight,
        expert_table,
        gate_weight[0],
        up_weight[0],
        down_weight[0],
    )
    return out.reshape(decode_hidden.shape)


def solution(mesh):
    placed = (
        P("groups", "ep", None),
        P(("groups", "ep"), "rep", None),
        P(("groups", "ep"), None, "rep"),
        P(),
        P(None, "rep"),
        P("rep", None),
        P(),
        P(("ep", "rep"), None, None),
        P(("ep", "rep"), None, None),
        P(("ep", "rep"), None, None),
        P(),
        P("ep", "rep"),
        P("groups"),
    )
    return jax.shard_map(
        local,
        mesh=mesh,
        in_specs=placed,
        out_specs=P(("groups", "ep"), "rep", None),
        check_vma=False,
    )
```

```python
import functools
import math

import jax
import jax.numpy as jnp
from jax import lax
from jax.experimental import pallas as pl
from jax.experimental.pallas import tpu as pltpu
from jax.sharding import PartitionSpec as P

HEAD_DIM = 128
QUERY_HEADS = 16
KEY_VALUE_HEADS = 4
GROUP_PROMPTS = 4
CAP = 2

EPS = 1e-06
THETA = 1000000.0
MESH = pl.DeviceIdType.MESH
F32 = jnp.float32
BF16 = jnp.bfloat16


def dot(a, b):
    return jnp.dot(a, b, preferred_element_type=F32)


def dot_t(a, b):
    return lax.dot_general(a, b, (((0,), (0,)), ((), ())), preferred_element_type=F32)


def one_hot(hit):
    return jnp.where(hit, 1.0, 0.0).astype(BF16)


SHARED_ROWS = 1024
DIRECT = 512
FAR = 4
CHUNKS = 2


def layer_kernel(
    nx, ne, prompt_hbm, hidden_hbm, query_hbm, gain_ref, moe_gain_ref, lengths_ref, ids_ref, idrow_ref,
    kvw_hbm, ow_hbm, table_hbm, gate_hbm, up_hbm, down_hbm, out_ref,
    prompt_ref, hidden_ref, query_ref,
    kvw, ow, table, picked, hn, pn, qf, qt, skv, dkv, spk, pkv, pf, kp, vp, att, full, mixed_ref, top_p, total_p, summed_p,
    gate, up, down, normed, hid, gate_acc, up_acc,
    s0, s1, r0, r1, t0, t1, q0, q1, o0, o1, b0, b1, c0, c1, f0, f1,
    lsem, wsem, ring_send, ring_recv, dd_send, dd_recv, xs, xr, msend, mrecv,
):
    e, x, g = lax.axis_index("ep"), lax.axis_index("rep"), lax.axis_index("groups")
    ny = ne // 2
    y, c = e // 2, lax.rem(e, 2)
    rows, width = hidden_hbm.shape
    shared = SHARED_ROWS
    piece = shared // ne
    sub = (width - shared) // 4
    orow = ow.shape[1] // ne
    half = (width - DIRECT) // 2
    lines = ow.shape[1] // 4
    spread_cols = pl.ds(DIRECT, width - DIRECT)
    plen = prompt_hbm.shape[0] // GROUP_PROMPTS
    own_prompt = e // (ne // GROUP_PROMPTS)
    seqs = 16

    def sub_rows(core, s):
        return pl.ds(pl.multiple_of(shared + core * (2 * sub) + s * sub, 16), sub)

    def piece_rows(k, size, unit):
        return pl.ds(pl.multiple_of(k * unit, 16), size)

    loads = [
        pltpu.make_async_copy(
            kvw_hbm.at[pl.ds(shared, width - shared)], kvw.at[x, pl.ds(shared, width - shared)], lsem.at[0]
        ),
        pltpu.make_async_copy(
            kvw_hbm.at[piece_rows(e, piece, piece)], kvw.at[x, piece_rows(e, piece, piece)], lsem.at[1]
        ),
        pltpu.make_async_copy(
            ow_hbm.at[piece_rows(e, orow, orow), spread_cols],
            ow.at[FAR, piece_rows(e, orow, orow), spread_cols],
            lsem.at[2],
        ),
        pltpu.make_async_copy(ow_hbm.at[:, pl.ds(0, DIRECT)], ow.at[FAR, :, pl.ds(0, DIRECT)], lsem.at[7]),
    ]
    late = [
        pltpu.make_async_copy(hidden_hbm, hidden_ref, lsem.at[3]),
        pltpu.make_async_copy(prompt_hbm, prompt_ref, lsem.at[4]),
        pltpu.make_async_copy(query_hbm, query_ref, lsem.at[5]),
        pltpu.make_async_copy(table_hbm, table, lsem.at[6]),
    ]
    weights = [
        pltpu.make_async_copy(gate_hbm, gate, wsem.at[0]),
        pltpu.make_async_copy(up_hbm, up, wsem.at[1]),
        pltpu.make_async_copy(down_hbm, down, wsem.at[2]),
    ]
    for load in loads + late:
        load.start()

    sibling = (g, 2 * y + 1 - c, x)

    def at_x(k):
        return (g, e, lax.rem(x + k + nx, nx))

    def at_y(k):
        return (g, 2 * lax.rem(y + k + ny, ny) + c, x)

    barrier = pltpu.get_barrier_semaphore()
    for i in range(1, nx):
        pl.semaphore_signal(barrier, inc=1, device_id=at_x(i), device_id_type=MESH)
    for i in range(1, ne):
        peer = (g, lax.rem(e + i, ne), x)
        pl.semaphore_signal(barrier, inc=1, device_id=peer, device_id_type=MESH)

    class Ring:
        def __init__(self, number, along, sign, hops, place, total, mate):
            self.along, self.sign, self.hops, self.place = along, sign, hops, place
            self.number, self.total, self.mate = number, total, mate

        def origin(self, h):
            me, n = (x, nx) if self.along == "x" else (y, ny)
            return lax.rem(me - self.sign * h + n, n)

        def at(self, h):
            return self.place(self.origin(h), (FAR - self.sign * h) % (2 * FAR))

        def go(self, h):
            ref = self.at(h)
            there = self.place(self.origin(h), (FAR - self.sign * (h + 1)) % (2 * FAR))
            to = at_x(self.sign) if self.along == "x" else at_y(self.sign)
            pltpu.make_async_remote_copy(
                ref, there, ring_send.at[self.number], ring_recv.at[self.number, h],
                device_id=to, device_id_type=MESH,
            ).start()

        def event(self, h):
            if h > self.hops:
                return
            ref = self.at(h)
            pltpu.make_async_copy(ref, ref, ring_recv.at[self.number, h - 1]).wait()
            if h < self.hops:
                self.go(h)
            if self.mate is not None:
                to_mate(ref, self.mate)

        def finish(self):
            ref = self.total(self.hops)
            pltpu.make_async_copy(ref, ref, ring_send.at[self.number]).wait()

    def to_mate(ref, k):
        pltpu.make_async_remote_copy(
            ref, ref, dd_send.at[k], dd_recv.at[k], device_id=sibling, device_id_type=MESH
        ).start()

    def mate_done(ref, k):
        pltpu.make_async_copy(ref, ref, dd_send.at[k]).wait()
        pltpu.make_async_copy(ref, ref, dd_recv.at[k]).wait()

    def pair(base, along, more, place, total, mate):
        return [
            Ring(base, along, 1, 4 if more else 3, place, total, mate),
            Ring(base + 1, along, -1, 3 if more else 4, place, total, mate),
        ]

    def kv_pair(base, s):
        return pair(
            base, "x", s == 0,
            lambda j, i: kvw.at[j, sub_rows(c, s)],
            lambda n: kvw.at[pl.ds(0, n), pl.ds(0, sub)],
            0,
        )

    def kv_spread(base, s):
        slices = pl.ds(4 * s, 4)
        return pair(
            base, "y", s == 0,
            lambda k, i: kvw.at[slices, piece_rows(2 * k + c, piece, piece)],
            lambda n: kvw.at[slices, pl.ds(0, n * piece)],
            3,
        )

    def spread_pair(base, s):
        return pair(
            base, "x", s == 0,
            lambda j, i: ow.at[i, piece_rows(e, orow, orow), pl.ds(DIRECT + s * half, half)],
            lambda n: ow.at[pl.ds(0, n), pl.ds(0, orow), pl.ds(0, half)],
            None,
        )

    def ow_pair(base, more, first, n_slices):
        slices = pl.ds(first, n_slices)
        return pair(
            base, "y", more,
            lambda k, i: ow.at[
                slices, piece_rows(2 * k + c, orow, orow), spread_cols
            ],
            lambda n: ow.at[slices, pl.ds(0, n * orow), spread_cols],
            1,
        )

    def direct_pair(base, s):
        return pair(
            base, "x", s == 0,
            lambda j, i: ow.at[
                i, pl.ds(pl.multiple_of(c * (2 * lines) + s * lines, 16), lines), pl.ds(0, DIRECT)
            ],
            lambda n: ow.at[pl.ds(0, n), pl.ds(0, lines), pl.ds(0, DIRECT)],
            4,
        )

    straight = direct_pair(18, 0) + direct_pair(20, 1)
    kv_x = kv_pair(0, 0) + kv_pair(2, 1)
    kv_y = kv_spread(14, 0) + kv_spread(16, 1)
    ow_x = spread_pair(4, 0) + spread_pair(6, 1)
    near = ow_pair(8, True, FAR - 1, 3)
    rest = ow_pair(10, False, 0, FAR - 1) + ow_pair(12, True, FAR + 2, nx - FAR - 2)

    def events(rings, h):
        for ring in rings:
            ring.event(h)

    def begin(rings, slices):
        for ring in rings:
            ring.go(0)
        to_mate(ow.at[slices, piece_rows(e, orow, orow), spread_cols], 1)

    def normalised(ref, out):
        widened = ref[...].astype(F32)
        scale = lax.rsqrt(jnp.mean(widened * widened, axis=-1, keepdims=True) + EPS)
        out[...] = (widened * scale * gain_ref[...]).astype(BF16)

    with jax.named_scope("enter"):
        for load in loads:
            load.wait()
        pl.semaphore_wait(barrier, nx + ne - 2)

    own_piece = piece_rows(e, piece, piece)
    for i in range(1, nx):
        ref = kvw.at[x, own_piece]
        pltpu.make_async_remote_copy(
            ref, ref, xs.at[0], xr.at[0], device_id=at_x(i), device_id_type=MESH
        ).start()
    for ring in kv_x:
        ring.go(0)
    for load in late:
        load.wait()
    normalised(hidden_ref, hn)
    with jax.named_scope("spread_wait"):
        ref = kvw.at[pl.ds(0, nx - 1), pl.ds(0, piece)]
        pltpu.make_async_copy(ref, ref, xs.at[0]).wait()
        pltpu.make_async_copy(ref, ref, xr.at[0]).wait()
    for ring in kv_y:
        ring.go(0)
    for ring in ow_x:
        ring.go(0)
    for s in range(2):
        to_mate(kvw.at[pl.ds(4 * s, 4), own_piece], 3)
    for h in range(1, 5):
        with jax.named_scope(f"kv_x#h={h}"):
            events(kv_x, h)
        if h == 4:
            with jax.named_scope("ow_x#h=4"):
                events(ow_x, 4)
            begin(rest, pl.ds(0, FAR - 1))
            to_mate(ow.at[pl.ds(FAR + 2, nx - FAR - 2), piece_rows(e, orow, orow), spread_cols], 1)
        with jax.named_scope(f"kv_y#h={h}"):
            events(kv_y, h)
        if h == 3:
            begin(near, pl.ds(FAR - 1, 3))
            for ring in straight:
                ring.go(0)
        if h < 4:
            with jax.named_scope(f"ow_x#h={h}"):
                events(ow_x, h)
        if h == 1:
            normalised(prompt_ref, pn)
            for k in range(2):
                qf[k] = query_ref[:, pl.ds(k * HEAD_DIM, HEAD_DIM)].astype(F32)
            for weight in weights:
                weight.start()
        if h == 2:
            for t in range(nx):
                for k in range(2):
                    cols = pl.ds(k * HEAD_DIM, HEAD_DIM)
                    qt[t, :, cols] = qf[k, pl.ds(t, rows, stride=nx), :].astype(BF16)
    with jax.named_scope("kv_mate"):
        mate_done(kvw.at[pl.ds(0, nx - 1), pl.ds(0, 2 * sub)], 0)
        mate_done(kvw.at[pl.ds(0, nx), pl.ds(0, ny * piece)], 3)

    length = lengths_ref[own_prompt]
    half_dim = HEAD_DIM // 2

    def turns(count, positions):
        lane = lax.broadcasted_iota(jnp.int32, (count, HEAD_DIM), 1)
        freq = jnp.exp(lax.rem(lane, half_dim).astype(F32) * (-2.0 * math.log(THETA) / HEAD_DIM))
        angles = positions.astype(F32) * freq
        sine = jnp.sin(angles)
        return jnp.cos(angles), jnp.where(lane < half_dim, -sine, sine)

    def turned(keys, cosine, sine):
        return keys * cosine + pltpu.roll(keys, half_dim, 1) * sine

    cosine, sine = turns(8, jnp.full((8, HEAD_DIM), length + x, jnp.int32))
    cosine, sine = cosine[0:1], sine[0:1]
    def own_kv(head):
        skv[head, 0] = turned(dot(hn[...], kvw[2 * head]), cosine, sine).astype(BF16)
        skv[head, 1] = dot(hn[...], kvw[2 * head + 1]).astype(BF16)

    def send_kv(head, to):
        pltpu.make_async_remote_copy(
            skv.at[head], dkv.at[x], xs.at[1], xr.at[1], device_id=(g, e, to), device_id_type=MESH
        ).start()

    with jax.named_scope("straight#h=1"):
        events(straight, 1)
    with jax.named_scope("own_kv"):
        for i in (2, 1, 3, 0):
            head = lax.rem(x // 2 + i, KEY_VALUE_HEADS)
            own_kv(head)
            if i:
                send_kv(head, 2 * head)
                send_kv(head, 2 * head + 1)
            else:
                send_kv(head, x + 1 - 2 * lax.rem(x, 2))
    dkv[x] = skv[x // 2]

    count = GROUP_PROMPTS * plen
    line = lax.broadcasted_iota(jnp.int32, (count, HEAD_DIM), 0)
    pcos, psin = turns(count, e * plen + lax.rem(line, plen))
    head = x // 2
    with jax.named_scope("prompt_kv"):
        pkey = turned(dot(pn[...], kvw[2 * head]), pcos, psin)
        pval = dot(pn[...], kvw[2 * head + 1])
    spk[:, 0] = pkey.reshape(GROUP_PROMPTS, plen, HEAD_DIM).astype(BF16)
    spk[:, 1] = pval.reshape(GROUP_PROMPTS, plen, HEAD_DIM).astype(BF16)
    per = ny // GROUP_PROMPTS
    for i in range(1, ny):
        to = lax.rem(y + i, ny)
        pltpu.make_async_remote_copy(
            spk.at[to // per], pkv.at[c, y], xs.at[2], xr.at[2],
            device_id=(g, 2 * to + c, x), device_id_type=MESH,
        ).start()
    pkv[c, y] = spk[y // per]
    with jax.named_scope("near#h=1"):
        events(near, 1)

    def look(i, carry):
        at = lax.div(ids_ref[i], 128)
        picked[pl.ds(i, 1), :] = table[pl.ds(at, 1), :]
        return carry

    with jax.named_scope("look"):
        lax.fori_loop(0, rows, look, 0)
    with jax.named_scope("prompt_wait"):
        ref = pkv.at[0, pl.ds(0, ny - 1)]
        pltpu.make_async_copy(ref, ref, xs.at[2]).wait()
        pltpu.make_async_copy(ref, ref, xr.at[2]).wait()
        to_mate(pkv.at[c], 2)
        mate_done(pkv.at[0], 2)
    for k in range(2):
        for core in range(2):
            for row in range(ny):
                start = (2 * row + core) * plen
                pf[pl.ds(start, plen), :] = pkv[core, row, k].astype(F32)
        (kp if k == 0 else vp)[...] = pf[...].astype(BF16)

    keys = kp.shape[0]
    block = 2 * nx * seqs
    scale = HEAD_DIM ** (-0.5)
    valid = lax.broadcasted_iota(jnp.int32, (block, keys), 1) < length
    r = lax.rem(lax.broadcasted_iota(jnp.int32, (block, nx * seqs), 0), nx * seqs)
    k = lax.broadcasted_iota(jnp.int32, (block, nx * seqs), 1)
    own = (lax.rem(r, seqs) == lax.rem(k, seqs)) & (k // seqs <= r // seqs)

    def nt(a, b):
        return lax.dot_general(a, b, (((1,), (1,)), ((), ())), preferred_element_type=F32)

    def asked(pick):
        return jnp.concatenate(
            [qt[:, pick, pl.ds(h * HEAD_DIM, HEAD_DIM)].reshape(nx * seqs, HEAD_DIM) for h in range(2)], axis=0
        )

    def twice(body, i, carry):
        return body(2 * i + 1, body(2 * i, carry))

    def attend_prompt(j, carry):
        pick = pl.ds(pl.multiple_of(j * seqs, seqs), seqs)
        scores = jnp.where(valid, nt(asked(pick), kp[...]) * scale, -1e30)
        top = jnp.max(scores, axis=1, keepdims=True)
        weight = jnp.where(valid, jnp.exp(scores - top), 0.0)
        top_p[j] = top
        total_p[j] = jnp.sum(weight, axis=1, keepdims=True)
        summed_p[j] = dot(weight.astype(BF16), vp[...])
        return carry

    def attend(j, carry):
        pick = pl.ds(pl.multiple_of(j * seqs, seqs), seqs)
        scores = nt(asked(pick), dkv[:, 0, pick].reshape(nx * seqs, HEAD_DIM)) * scale
        scores = jnp.where(own, scores, -1e30)
        top = jnp.maximum(top_p[j], jnp.max(scores, axis=1, keepdims=True))
        weight = jnp.where(own, jnp.exp(scores - top), 0.0)
        decay = jnp.exp(top_p[j] - top)
        total = total_p[j] * decay + jnp.sum(weight, axis=1, keepdims=True)
        summed = summed_p[j] * decay
        summed = summed + dot(weight.astype(BF16), dkv[:, 1, pick].reshape(nx * seqs, HEAD_DIM))
        result = (summed / total).astype(BF16)
        for h in range(2):
            att[:, pick, pl.ds(h * HEAD_DIM, HEAD_DIM)] = result[h * nx * seqs:(h + 1) * nx * seqs].reshape(
                nx, seqs, HEAD_DIM
            )
        return carry

    with jax.named_scope("straight#h=2"):
        events(straight, 2)
    with jax.named_scope("rest#h=1"):
        events(rest, 1)
    with jax.named_scope("attend_prompt"):
        lax.fori_loop(0, rows // seqs // 2, functools.partial(twice, attend_prompt), 0)
    with jax.named_scope("near#h=2"):
        events(near, 2)
    with jax.named_scope("kv_wait"):
        ref = dkv.at[pl.ds(0, nx - 1)]
        pltpu.make_async_copy(ref, ref, xs.at[1]).wait()
        pltpu.make_async_copy(ref, ref, xr.at[1]).wait()
    with jax.named_scope("attend"):
        lax.fori_loop(0, rows // seqs // 2, functools.partial(twice, attend), 0)
    with jax.named_scope("straight#h=3"):
        events(straight, 3)
    for i in range(1, nx):
        to = lax.rem(x + i, nx)
        pltpu.make_async_remote_copy(
            att.at[to], full.at[x], xs.at[3], xr.at[3], device_id=(g, e, to), device_id_type=MESH
        ).start()
    full[x] = att[x]
    with jax.named_scope("near#h=3"):
        events(near, 3)
    with jax.named_scope("rest#h=2"):
        events(rest, 2)
    with jax.named_scope("near#h=4"):
        events(near, 4)
    with jax.named_scope("rest#h=3"):
        events(rest, 3)
    with jax.named_scope("straight#h=4"):
        events(straight, 4)
    with jax.named_scope("rest#h=4"):
        events(rest, 4)
    with jax.named_scope("full_wait"):
        ref = full.at[pl.ds(0, nx - 1)]
        pltpu.make_async_copy(ref, ref, xs.at[3]).wait()
        pltpu.make_async_copy(ref, ref, xr.at[3]).wait()
    with jax.named_scope("ow_mate"):
        mate_done(ow.at[pl.ds(0, nx), pl.ds(0, ny * orow), spread_cols], 1)
        mate_done(ow.at[pl.ds(0, nx - 1), pl.ds(0, 2 * lines), pl.ds(0, DIRECT)], 4)

    tile = 512

    def project(i, carry):
        cols = pl.ds(pl.multiple_of(i * tile, tile), tile)
        total = dot(full[x], ow[FAR, :, cols])
        for k in range(1, nx):
            total = total + dot(full[lax.rem(x + k, nx)], ow[(FAR + k) % nx, :, cols])
        mixed_ref[:, cols] = (hidden_ref[:, cols].astype(F32) + total).astype(BF16)
        return carry

    with jax.named_scope("project"):
        lax.fori_loop(0, width // tile, project, 0)
    lane = lax.broadcasted_iota(jnp.int32, (rows, rows), 1)
    line = lax.broadcasted_iota(jnp.int32, (rows, rows), 0)
    idcol = jnp.sum(jnp.where(lane == line, idrow_ref[...], 0), axis=1, keepdims=True)
    col = jnp.sum(jnp.where(lane == lax.rem(idcol, 128), picked[...], 0), axis=1, keepdims=True)
    row = jnp.sum(jnp.where(lane == line, col, 0), axis=0, keepdims=True)
    earlier = jnp.where((row == col) & (line < lane), 1, 0)
    rank = jnp.sum(earlier, axis=0, keepdims=True)
    cells = nx * ne
    slot = lax.broadcasted_iota(jnp.int32, (cells, rows), 0)
    swapped = lax.rem(slot, ne) * nx + slot // ne
    pick0 = one_hot((swapped == row) & (rank == 0))
    pick1 = one_hot((slot == row) & (rank == 1))
    here = lax.broadcasted_iota(jnp.int32, (cells, cells), 0)
    there = lax.broadcasted_iota(jnp.int32, (cells, cells), 1)
    to_ex = one_hot(there == lax.rem(here, nx) * ne + here // nx)
    to_xe = one_hot(there == lax.rem(here, ne) * nx + here // ne)

    with jax.named_scope("moe_norm"):
        widened = mixed_ref[...].astype(F32)
        scale = lax.rsqrt(jnp.mean(widened * widened, axis=-1, keepdims=True) + EPS)
        normed[...] = (widened * scale * moe_gain_ref[...]).astype(BF16)

    part = width // CHUNKS
    tile = 512

    def tiles(chunk, body):
        def step(i, carry):
            body(pl.ds(pl.multiple_of(chunk * part + i * tile, tile), tile))
            return carry

        lax.fori_loop(0, part // tile, step, 0)

    def put(ref, cols, value):
        ref[:, :, cols] = value.reshape(ref.shape[0], ref.shape[1], tile).astype(BF16)

    def get(ref, cols):
        return ref[:, :, cols].astype(F32).reshape(cells, tile).astype(BF16)

    def send(src, dst, k, chunk):
        n = dst.shape[0]
        me = x if n == nx else e
        cols = pl.ds(chunk * part, part)
        for i in range(1, n):
            to = lax.rem(me + i, n)
            pltpu.make_async_remote_copy(
                src.at[to, :, cols], dst.at[me, :, cols], msend.at[k, chunk], mrecv.at[k, chunk],
                device_id=(g, e, to) if n == nx else (g, to, x), device_id_type=MESH,
            ).start()
        dst[me, :, cols] = src[me, :, cols]

    def arrive(dst, k, chunk):
        ref = dst.at[pl.ds(0, dst.shape[0] - 1), :, pl.ds(chunk * part, part)]
        pltpu.make_async_copy(ref, ref, msend.at[k, chunk]).wait()
        pltpu.make_async_copy(ref, ref, mrecv.at[k, chunk]).wait()

    def two_phases(base, a0, m0, n0, d0, a1, m1, n1, d1, order0, order1, fill):
        for chunk in range(CHUNKS):
            with jax.named_scope("fill"):
                fill(chunk)
            send(a0, m0, base, chunk)
            send(a1, m1, base + 1, chunk)
        for chunk in range(CHUNKS):
            with jax.named_scope("wait_first"):
                arrive(m0, base, chunk)
            with jax.named_scope("permute"):
                tiles(chunk, lambda cols: put(n0, cols, dot(order0, get(m0, cols))))
            send(n0, d0, base + 2, chunk)
            with jax.named_scope("wait_first"):
                arrive(m1, base + 1, chunk)
            with jax.named_scope("permute"):
                tiles(chunk, lambda cols: put(n1, cols, dot(order1, get(m1, cols))))
            send(n1, d1, base + 3, chunk)

    def scatter(chunk):
        def body(cols):
            put(s0, cols, dot(pick0, normed[:, cols]))
            put(s1, cols, dot(pick1, normed[:, cols]))

        tiles(chunk, body)

    two_phases(0, s0, r0, t0, q0, s1, r1, t1, q1, to_ex, to_xe, scatter)
    with jax.named_scope("weights"):
        for weight in weights:
            weight.wait()

    ff = gate.shape[1]
    ftile = 256
    for chunk in range(CHUNKS):
        with jax.named_scope("wait_second"):
            arrive(q0, 2, chunk)
            arrive(q1, 3, chunk)
        with jax.named_scope("inner"):
            cols = pl.ds(chunk * part, part)
            tokens = jnp.concatenate(
                [q[:, :, cols].astype(F32).reshape(cells, part).astype(BF16) for q in (q0, q1)], axis=0
            )
            if chunk == 0:
                gate_acc[...] = dot(tokens, gate[cols, :])
                up_acc[...] = dot(tokens, up[cols, :])
            else:
                gate_acc[...] += dot(tokens, gate[cols, :])
                up_acc[...] += dot(tokens, up[cols, :])
    with jax.named_scope("silu"):
        hid[...] = (jax.nn.silu(gate_acc[...]) * up_acc[...]).astype(BF16)

    def outer(chunk):
        def body(cols):
            put(o0, cols, dot(hid[pl.ds(0, cells), :], down[:, cols]))
            put(o1, cols, dot(hid[pl.ds(cells, cells), :], down[:, cols]))

        tiles(chunk, body)

    two_phases(4, o0, b0, c0, f0, o1, b1, c1, f1, to_xe, to_ex, outer)
    for chunk in range(CHUNKS):
        with jax.named_scope("wait_second"):
            arrive(f0, 6, chunk)
            arrive(f1, 7, chunk)

        def combine(cols):
            moe = dot_t(pick0, get(f0, cols)) + dot_t(pick1, get(f1, cols))
            out_ref[:, cols] = (mixed_ref[:, cols].astype(F32) + moe).astype(BF16)

        with jax.named_scope("combine"):
            tiles(chunk, combine)
    for ring in kv_x + kv_y + ow_x + near + rest + straight:
        ring.finish()


def layer(prompt, hidden, queries, gain, moe_gain, lengths, ids, kvw, ow, expert_table, gate, up, down):
    nx, ne = lax.axis_size("rep"), lax.axis_size("ep")
    rows, width = hidden.shape
    count = prompt.shape[0]
    plen = count // GROUP_PROMPTS
    keys = plen * ne
    ff = gate.shape[1]
    vmem, any_ = pl.BlockSpec(memory_space=pltpu.VMEM), pl.BlockSpec(memory_space=pl.ANY)
    smem = pl.BlockSpec(memory_space=pltpu.SMEM)
    cols = queries.shape[1]
    table = expert_table.reshape(-1, 128)
    sem = pltpu.SemaphoreType.DMA
    xe = pltpu.VMEM((nx, ne, width), BF16)
    ex = pltpu.VMEM((ne, nx, width), BF16)
    return pl.pallas_call(
        functools.partial(layer_kernel, nx, ne),
        out_shape=jax.ShapeDtypeStruct((rows, width), BF16),
        in_specs=[any_] * 3 + [vmem] * 2 + [smem] * 2 + [vmem] + [any_] * 6,
        out_specs=vmem,
        scratch_shapes=[
            pltpu.VMEM(prompt.shape, BF16),
            pltpu.VMEM(hidden.shape, BF16),
            pltpu.VMEM(queries.shape, BF16),
            pltpu.VMEM((nx,) + kvw.shape, BF16),
            pltpu.VMEM((nx,) + ow.shape, BF16),
            pltpu.VMEM(table.shape, jnp.int32),
            pltpu.VMEM((rows, 128), jnp.int32),
            pltpu.VMEM((rows, width), BF16),
            pltpu.VMEM((count, width), BF16),
            pltpu.VMEM((2, queries.shape[0], HEAD_DIM), F32),
            pltpu.VMEM((nx, rows, cols), BF16),
            pltpu.VMEM((KEY_VALUE_HEADS, 2, rows, HEAD_DIM), BF16),
            pltpu.VMEM((nx, 2, rows, HEAD_DIM), BF16),
            pltpu.VMEM((GROUP_PROMPTS, 2, plen, HEAD_DIM), BF16),
            pltpu.VMEM((2, ne // 2, 2, plen, HEAD_DIM), BF16),
            pltpu.VMEM((keys, HEAD_DIM), F32),
            pltpu.VMEM((keys, HEAD_DIM), BF16),
            pltpu.VMEM((keys, HEAD_DIM), BF16),
            pltpu.VMEM((nx, rows, cols), BF16),
            pltpu.VMEM((nx, rows, cols), BF16),
            pltpu.VMEM((rows, width), BF16),
            pltpu.VMEM((rows // 16, 32 * nx, 1), F32),
            pltpu.VMEM((rows // 16, 32 * nx, 1), F32),
            pltpu.VMEM((rows // 16, 32 * nx, HEAD_DIM), F32),
            pltpu.VMEM(gate.shape, BF16), pltpu.VMEM(up.shape, BF16), pltpu.VMEM(down.shape, BF16),
            pltpu.VMEM((rows, width), BF16), pltpu.VMEM((2 * nx * ne, ff), BF16),
            pltpu.VMEM((2 * nx * ne, ff), F32), pltpu.VMEM((2 * nx * ne, ff), F32),
            xe, ex, xe, ex, ex, xe, ex, xe, ex, xe, ex, xe, xe, ex, xe, ex,
            sem((8,)), sem((3,)), sem((22,)), sem((22, 4)), sem((5,)), sem((5,)), sem((4,)), sem((4,)),
            sem((8, CHUNKS)), sem((8, CHUNKS)),
        ],
        compiler_params=pltpu.CompilerParams(
            collective_id=0, has_side_effects=True, vmem_limit_bytes=67043328
        ),
        name="layer",
    )(
        prompt, hidden, queries, gain.reshape(1, width), moe_gain.reshape(1, width), lengths,
        ids.reshape(rows), ids.reshape(1, rows), kvw, ow, table, gate, up, down,
    )


def local(
    prompt_hidden,
    decode_hidden,
    queries,
    attn_gain,
    key_value_weight,
    out_weight,
    moe_gain,
    gate_weight,
    up_weight,
    down_weight,
    expert_table,
    token_ids,
    prompt_lengths,
):
    width = decode_hidden.shape[2]
    out = layer(
        prompt_hidden.reshape(-1, width),
        decode_hidden.reshape(-1, width),
        queries.reshape(-1, queries.shape[2]),
        attn_gain,
        moe_gain,
        prompt_lengths,
        token_ids,
        key_value_weight,
        out_weight,
        expert_table,
        gate_weight[0],
        up_weight[0],
        down_weight[0],
    )
    return out.reshape(decode_hidden.shape)


def solution(mesh):
    placed = (
        P("groups", "ep", None),
        P(("groups", "ep"), "rep", None),
        P(("groups", "ep"), None, "rep"),
        P(),
        P(None, "rep"),
        P("rep", None),
        P(),
        P(("ep", "rep"), None, None),
        P(("ep", "rep"), None, None),
        P(("ep", "rep"), None, None),
        P(),
        P("ep", "rep"),
        P("groups"),
    )
    return jax.shard_map(
        local,
        mesh=mesh,
        in_specs=placed,
        out_specs=P(("groups", "ep"), "rep", None),
        check_vma=False,
    )
```

```python
import functools
import math

import jax
import jax.numpy as jnp
from jax import lax
from jax.experimental import pallas as pl
from jax.experimental.pallas import tpu as pltpu
from jax.sharding import PartitionSpec as P

HEAD_DIM = 128
QUERY_HEADS = 16
KEY_VALUE_HEADS = 4
GROUP_PROMPTS = 4
CAP = 2

EPS = 1e-06
THETA = 1000000.0
MESH = pl.DeviceIdType.MESH
F32 = jnp.float32
BF16 = jnp.bfloat16


def dot(a, b):
    return jnp.dot(a, b, preferred_element_type=F32)


def dot_t(a, b):
    return lax.dot_general(a, b, (((0,), (0,)), ((), ())), preferred_element_type=F32)


def one_hot(hit):
    return jnp.where(hit, 1.0, 0.0).astype(BF16)


SHARED_ROWS = 1024
DIRECT = 512
FAR = 4
CHUNKS = 4


def layer_kernel(
    nx, ne, prompt_hbm, hidden_hbm, query_hbm, gain_ref, moe_gain_ref, lengths_ref, ids_ref, idrow_ref,
    kvw_hbm, ow_hbm, table_hbm, gate_hbm, up_hbm, down_hbm, out_ref,
    prompt_ref, hidden_ref, query_ref,
    kvw, ow, table, picked, hn, pn, qf, qt, skv, dkv, spk, pkv, pf, kp, vp, att, full, mixed_ref, top_p, total_p, summed_p,
    gate, up, down, normed, hid, gate_acc, up_acc,
    s0, s1, r0, r1, t0, t1, q0, q1, o0, o1, b0, b1, c0, c1, f0, f1,
    lsem, wsem, ring_send, ring_recv, dd_send, dd_recv, xs, xr, msend, mrecv,
):
    e, x, g = lax.axis_index("ep"), lax.axis_index("rep"), lax.axis_index("groups")
    ny = ne // 2
    y, c = e // 2, lax.rem(e, 2)
    rows, width = hidden_hbm.shape
    shared = SHARED_ROWS
    piece = shared // ne
    sub = (width - shared) // 4
    orow = ow.shape[1] // ne
    half = (width - DIRECT) // 2
    lines = ow.shape[1] // 4
    spread_cols = pl.ds(DIRECT, width - DIRECT)
    plen = prompt_hbm.shape[0] // GROUP_PROMPTS
    own_prompt = e // (ne // GROUP_PROMPTS)
    seqs = 16

    def sub_rows(core, s):
        return pl.ds(pl.multiple_of(shared + core * (2 * sub) + s * sub, 16), sub)

    def piece_rows(k, size, unit):
        return pl.ds(pl.multiple_of(k * unit, 16), size)

    loads = [
        pltpu.make_async_copy(
            kvw_hbm.at[pl.ds(shared, width - shared)], kvw.at[x, pl.ds(shared, width - shared)], lsem.at[0]
        ),
        pltpu.make_async_copy(
            kvw_hbm.at[piece_rows(e, piece, piece)], kvw.at[x, piece_rows(e, piece, piece)], lsem.at[1]
        ),
        pltpu.make_async_copy(
            ow_hbm.at[piece_rows(e, orow, orow), spread_cols],
            ow.at[FAR, piece_rows(e, orow, orow), spread_cols],
            lsem.at[2],
        ),
        pltpu.make_async_copy(ow_hbm.at[:, pl.ds(0, DIRECT)], ow.at[FAR, :, pl.ds(0, DIRECT)], lsem.at[7]),
    ]
    late = [
        pltpu.make_async_copy(hidden_hbm, hidden_ref, lsem.at[3]),
        pltpu.make_async_copy(prompt_hbm, prompt_ref, lsem.at[4]),
        pltpu.make_async_copy(query_hbm, query_ref, lsem.at[5]),
        pltpu.make_async_copy(table_hbm, table, lsem.at[6]),
    ]
    weights = [
        pltpu.make_async_copy(gate_hbm, gate, wsem.at[0]),
        pltpu.make_async_copy(up_hbm, up, wsem.at[1]),
        pltpu.make_async_copy(down_hbm, down, wsem.at[2]),
    ]
    for load in loads + late:
        load.start()

    sibling = (g, 2 * y + 1 - c, x)

    def at_x(k):
        return (g, e, lax.rem(x + k + nx, nx))

    def at_y(k):
        return (g, 2 * lax.rem(y + k + ny, ny) + c, x)

    barrier = pltpu.get_barrier_semaphore()
    for i in range(1, nx):
        pl.semaphore_signal(barrier, inc=1, device_id=at_x(i), device_id_type=MESH)
    for i in range(1, ne):
        peer = (g, lax.rem(e + i, ne), x)
        pl.semaphore_signal(barrier, inc=1, device_id=peer, device_id_type=MESH)

    class Ring:
        def __init__(self, number, along, sign, hops, place, total, mate):
            self.along, self.sign, self.hops, self.place = along, sign, hops, place
            self.number, self.total, self.mate = number, total, mate

        def origin(self, h):
            me, n = (x, nx) if self.along == "x" else (y, ny)
            return lax.rem(me - self.sign * h + n, n)

        def at(self, h):
            return self.place(self.origin(h), (FAR - self.sign * h) % (2 * FAR))

        def go(self, h):
            ref = self.at(h)
            there = self.place(self.origin(h), (FAR - self.sign * (h + 1)) % (2 * FAR))
            to = at_x(self.sign) if self.along == "x" else at_y(self.sign)
            pltpu.make_async_remote_copy(
                ref, there, ring_send.at[self.number], ring_recv.at[self.number, h],
                device_id=to, device_id_type=MESH,
            ).start()

        def event(self, h):
            if h > self.hops:
                return
            ref = self.at(h)
            pltpu.make_async_copy(ref, ref, ring_recv.at[self.number, h - 1]).wait()
            if h < self.hops:
                self.go(h)
            if self.mate is not None:
                to_mate(ref, self.mate)

        def finish(self):
            ref = self.total(self.hops)
            pltpu.make_async_copy(ref, ref, ring_send.at[self.number]).wait()

    def to_mate(ref, k):
        pltpu.make_async_remote_copy(
            ref, ref, dd_send.at[k], dd_recv.at[k], device_id=sibling, device_id_type=MESH
        ).start()

    def mate_done(ref, k):
        pltpu.make_async_copy(ref, ref, dd_send.at[k]).wait()
        pltpu.make_async_copy(ref, ref, dd_recv.at[k]).wait()

    def pair(base, along, more, place, total, mate):
        return [
            Ring(base, along, 1, 4 if more else 3, place, total, mate),
            Ring(base + 1, along, -1, 3 if more else 4, place, total, mate),
        ]

    def kv_pair(base, s):
        return pair(
            base, "x", s == 0,
            lambda j, i: kvw.at[j, sub_rows(c, s)],
            lambda n: kvw.at[pl.ds(0, n), pl.ds(0, sub)],
            0,
        )

    def kv_spread(base, s):
        slices = pl.ds(4 * s, 4)
        return pair(
            base, "y", s == 0,
            lambda k, i: kvw.at[slices, piece_rows(2 * k + c, piece, piece)],
            lambda n: kvw.at[slices, pl.ds(0, n * piece)],
            3,
        )

    def spread_pair(base, s):
        return pair(
            base, "x", s == 0,
            lambda j, i: ow.at[i, piece_rows(e, orow, orow), pl.ds(DIRECT + s * half, half)],
            lambda n: ow.at[pl.ds(0, n), pl.ds(0, orow), pl.ds(0, half)],
            None,
        )

    def ow_pair(base, more, first, n_slices):
        slices = pl.ds(first, n_slices)
        return pair(
            base, "y", more,
            lambda k, i: ow.at[
                slices, piece_rows(2 * k + c, orow, orow), spread_cols
            ],
            lambda n: ow.at[slices, pl.ds(0, n * orow), spread_cols],
            1,
        )

    def direct_pair(base, s):
        return pair(
            base, "x", s == 0,
            lambda j, i: ow.at[
                i, pl.ds(pl.multiple_of(c * (2 * lines) + s * lines, 16), lines), pl.ds(0, DIRECT)
            ],
            lambda n: ow.at[pl.ds(0, n), pl.ds(0, lines), pl.ds(0, DIRECT)],
            4,
        )

    straight = direct_pair(18, 0) + direct_pair(20, 1)
    kv_x = kv_pair(0, 0) + kv_pair(2, 1)
    kv_y = kv_spread(14, 0) + kv_spread(16, 1)
    ow_x = spread_pair(4, 0) + spread_pair(6, 1)
    near = ow_pair(8, True, FAR - 1, 3)
    rest = ow_pair(10, False, 0, FAR - 1) + ow_pair(12, True, FAR + 2, nx - FAR - 2)

    def events(rings, h):
        for ring in rings:
            ring.event(h)

    def begin(rings, slices):
        for ring in rings:
            ring.go(0)
        to_mate(ow.at[slices, piece_rows(e, orow, orow), spread_cols], 1)

    def normalised(ref, out):
        widened = ref[...].astype(F32)
        scale = lax.rsqrt(jnp.mean(widened * widened, axis=-1, keepdims=True) + EPS)
        out[...] = (widened * scale * gain_ref[...]).astype(BF16)

    with jax.named_scope("enter"):
        for load in loads:
            load.wait()
        pl.semaphore_wait(barrier, nx + ne - 2)

    own_piece = piece_rows(e, piece, piece)
    for i in range(1, nx):
        ref = kvw.at[x, own_piece]
        pltpu.make_async_remote_copy(
            ref, ref, xs.at[0], xr.at[0], device_id=at_x(i), device_id_type=MESH
        ).start()
    for ring in kv_x:
        ring.go(0)
    for load in late:
        load.wait()
    normalised(hidden_ref, hn)
    with jax.named_scope("spread_wait"):
        ref = kvw.at[pl.ds(0, nx - 1), pl.ds(0, piece)]
        pltpu.make_async_copy(ref, ref, xs.at[0]).wait()
        pltpu.make_async_copy(ref, ref, xr.at[0]).wait()
    for ring in kv_y:
        ring.go(0)
    for ring in ow_x:
        ring.go(0)
    for s in range(2):
        to_mate(kvw.at[pl.ds(4 * s, 4), own_piece], 3)
    for h in range(1, 5):
        with jax.named_scope(f"kv_x#h={h}"):
            events(kv_x, h)
        if h == 4:
            with jax.named_scope("ow_x#h=4"):
                events(ow_x, 4)
            begin(rest, pl.ds(0, FAR - 1))
            to_mate(ow.at[pl.ds(FAR + 2, nx - FAR - 2), piece_rows(e, orow, orow), spread_cols], 1)
        with jax.named_scope(f"kv_y#h={h}"):
            events(kv_y, h)
        if h == 3:
            begin(near, pl.ds(FAR - 1, 3))
            for ring in straight:
                ring.go(0)
        if h < 4:
            with jax.named_scope(f"ow_x#h={h}"):
                events(ow_x, h)
        if h == 1:
            normalised(prompt_ref, pn)
            for k in range(2):
                qf[k] = query_ref[:, pl.ds(k * HEAD_DIM, HEAD_DIM)].astype(F32)
            for weight in weights:
                weight.start()
        if h == 2:
            for t in range(nx):
                for k in range(2):
                    cols = pl.ds(k * HEAD_DIM, HEAD_DIM)
                    qt[t, :, cols] = qf[k, pl.ds(t, rows, stride=nx), :].astype(BF16)
    with jax.named_scope("kv_mate"):
        mate_done(kvw.at[pl.ds(0, nx - 1), pl.ds(0, 2 * sub)], 0)
        mate_done(kvw.at[pl.ds(0, nx), pl.ds(0, ny * piece)], 3)

    length = lengths_ref[own_prompt]
    half_dim = HEAD_DIM // 2

    def turns(count, positions):
        lane = lax.broadcasted_iota(jnp.int32, (count, HEAD_DIM), 1)
        freq = jnp.exp(lax.rem(lane, half_dim).astype(F32) * (-2.0 * math.log(THETA) / HEAD_DIM))
        angles = positions.astype(F32) * freq
        sine = jnp.sin(angles)
        return jnp.cos(angles), jnp.where(lane < half_dim, -sine, sine)

    def turned(keys, cosine, sine):
        return keys * cosine + pltpu.roll(keys, half_dim, 1) * sine

    cosine, sine = turns(8, jnp.full((8, HEAD_DIM), length + x, jnp.int32))
    cosine, sine = cosine[0:1], sine[0:1]
    def own_kv(head):
        skv[head, 0] = turned(dot(hn[...], kvw[2 * head]), cosine, sine).astype(BF16)
        skv[head, 1] = dot(hn[...], kvw[2 * head + 1]).astype(BF16)

    def send_kv(head, to):
        pltpu.make_async_remote_copy(
            skv.at[head], dkv.at[x], xs.at[1], xr.at[1], device_id=(g, e, to), device_id_type=MESH
        ).start()

    with jax.named_scope("straight#h=1"):
        events(straight, 1)
    with jax.named_scope("own_kv"):
        for i in (2, 1, 3, 0):
            head = lax.rem(x // 2 + i, KEY_VALUE_HEADS)
            own_kv(head)
            if i:
                send_kv(head, 2 * head)
                send_kv(head, 2 * head + 1)
            else:
                send_kv(head, x + 1 - 2 * lax.rem(x, 2))
    dkv[x] = skv[x // 2]

    count = GROUP_PROMPTS * plen
    line = lax.broadcasted_iota(jnp.int32, (count, HEAD_DIM), 0)
    pcos, psin = turns(count, e * plen + lax.rem(line, plen))
    head = x // 2
    with jax.named_scope("prompt_kv"):
        pkey = turned(dot(pn[...], kvw[2 * head]), pcos, psin)
        pval = dot(pn[...], kvw[2 * head + 1])
    spk[:, 0] = pkey.reshape(GROUP_PROMPTS, plen, HEAD_DIM).astype(BF16)
    spk[:, 1] = pval.reshape(GROUP_PROMPTS, plen, HEAD_DIM).astype(BF16)
    per = ny // GROUP_PROMPTS
    for i in range(1, ny):
        to = lax.rem(y + i, ny)
        pltpu.make_async_remote_copy(
            spk.at[to // per], pkv.at[c, y], xs.at[2], xr.at[2],
            device_id=(g, 2 * to + c, x), device_id_type=MESH,
        ).start()
    pkv[c, y] = spk[y // per]
    with jax.named_scope("near#h=1"):
        events(near, 1)

    def look(i, carry):
        at = lax.div(ids_ref[i], 128)
        picked[pl.ds(i, 1), :] = table[pl.ds(at, 1), :]
        return carry

    with jax.named_scope("look"):
        lax.fori_loop(0, rows, look, 0)
    with jax.named_scope("prompt_wait"):
        ref = pkv.at[0, pl.ds(0, ny - 1)]
        pltpu.make_async_copy(ref, ref, xs.at[2]).wait()
        pltpu.make_async_copy(ref, ref, xr.at[2]).wait()
        to_mate(pkv.at[c], 2)
        mate_done(pkv.at[0], 2)
    for k in range(2):
        for core in range(2):
            for row in range(ny):
                start = (2 * row + core) * plen
                pf[pl.ds(start, plen), :] = pkv[core, row, k].astype(F32)
        (kp if k == 0 else vp)[...] = pf[...].astype(BF16)

    keys = kp.shape[0]
    block = 2 * nx * seqs
    scale = HEAD_DIM ** (-0.5)
    valid = lax.broadcasted_iota(jnp.int32, (block, keys), 1) < length
    r = lax.rem(lax.broadcasted_iota(jnp.int32, (block, nx * seqs), 0), nx * seqs)
    k = lax.broadcasted_iota(jnp.int32, (block, nx * seqs), 1)
    own = (lax.rem(r, seqs) == lax.rem(k, seqs)) & (k // seqs <= r // seqs)

    def nt(a, b):
        return lax.dot_general(a, b, (((1,), (1,)), ((), ())), preferred_element_type=F32)

    def asked(pick):
        return jnp.concatenate(
            [qt[:, pick, pl.ds(h * HEAD_DIM, HEAD_DIM)].reshape(nx * seqs, HEAD_DIM) for h in range(2)], axis=0
        )

    def twice(body, i, carry):
        return body(2 * i + 1, body(2 * i, carry))

    def attend_prompt(j, carry):
        pick = pl.ds(pl.multiple_of(j * seqs, seqs), seqs)
        scores = jnp.where(valid, nt(asked(pick), kp[...]) * scale, -1e30)
        top = jnp.max(scores, axis=1, keepdims=True)
        weight = jnp.where(valid, jnp.exp(scores - top), 0.0)
        top_p[j] = top
        total_p[j] = jnp.sum(weight, axis=1, keepdims=True)
        summed_p[j] = dot(weight.astype(BF16), vp[...])
        return carry

    def attend(j, carry):
        pick = pl.ds(pl.multiple_of(j * seqs, seqs), seqs)
        scores = nt(asked(pick), dkv[:, 0, pick].reshape(nx * seqs, HEAD_DIM)) * scale
        scores = jnp.where(own, scores, -1e30)
        top = jnp.maximum(top_p[j], jnp.max(scores, axis=1, keepdims=True))
        weight = jnp.where(own, jnp.exp(scores - top), 0.0)
        decay = jnp.exp(top_p[j] - top)
        total = total_p[j] * decay + jnp.sum(weight, axis=1, keepdims=True)
        summed = summed_p[j] * decay
        summed = summed + dot(weight.astype(BF16), dkv[:, 1, pick].reshape(nx * seqs, HEAD_DIM))
        result = (summed / total).astype(BF16)
        for h in range(2):
            att[:, pick, pl.ds(h * HEAD_DIM, HEAD_DIM)] = result[h * nx * seqs:(h + 1) * nx * seqs].reshape(
                nx, seqs, HEAD_DIM
            )
        return carry

    with jax.named_scope("straight#h=2"):
        events(straight, 2)
    with jax.named_scope("rest#h=1"):
        events(rest, 1)
    with jax.named_scope("attend_prompt"):
        lax.fori_loop(0, rows // seqs // 2, functools.partial(twice, attend_prompt), 0)
    with jax.named_scope("near#h=2"):
        events(near, 2)
    with jax.named_scope("kv_wait"):
        ref = dkv.at[pl.ds(0, nx - 1)]
        pltpu.make_async_copy(ref, ref, xs.at[1]).wait()
        pltpu.make_async_copy(ref, ref, xr.at[1]).wait()
    with jax.named_scope("attend"):
        lax.fori_loop(0, rows // seqs // 2, functools.partial(twice, attend), 0)
    with jax.named_scope("straight#h=3"):
        events(straight, 3)
    for i in range(1, nx):
        to = lax.rem(x + i, nx)
        pltpu.make_async_remote_copy(
            att.at[to], full.at[x], xs.at[3], xr.at[3], device_id=(g, e, to), device_id_type=MESH
        ).start()
    full[x] = att[x]
    with jax.named_scope("near#h=3"):
        events(near, 3)
    with jax.named_scope("rest#h=2"):
        events(rest, 2)
    with jax.named_scope("near#h=4"):
        events(near, 4)
    with jax.named_scope("rest#h=3"):
        events(rest, 3)
    with jax.named_scope("straight#h=4"):
        events(straight, 4)
    with jax.named_scope("rest#h=4"):
        events(rest, 4)
    with jax.named_scope("full_wait"):
        ref = full.at[pl.ds(0, nx - 1)]
        pltpu.make_async_copy(ref, ref, xs.at[3]).wait()
        pltpu.make_async_copy(ref, ref, xr.at[3]).wait()
    with jax.named_scope("ow_mate"):
        mate_done(ow.at[pl.ds(0, nx), pl.ds(0, ny * orow), spread_cols], 1)
        mate_done(ow.at[pl.ds(0, nx - 1), pl.ds(0, 2 * lines), pl.ds(0, DIRECT)], 4)

    tile = 512

    def project(i, carry):
        cols = pl.ds(pl.multiple_of(i * tile, tile), tile)
        total = dot(full[x], ow[FAR, :, cols])
        for k in range(1, nx):
            total = total + dot(full[lax.rem(x + k, nx)], ow[(FAR + k) % nx, :, cols])
        mixed_ref[:, cols] = (hidden_ref[:, cols].astype(F32) + total).astype(BF16)
        return carry

    with jax.named_scope("project"):
        lax.fori_loop(0, width // tile, project, 0)
    lane = lax.broadcasted_iota(jnp.int32, (rows, rows), 1)
    line = lax.broadcasted_iota(jnp.int32, (rows, rows), 0)
    idcol = jnp.sum(jnp.where(lane == line, idrow_ref[...], 0), axis=1, keepdims=True)
    col = jnp.sum(jnp.where(lane == lax.rem(idcol, 128), picked[...], 0), axis=1, keepdims=True)
    row = jnp.sum(jnp.where(lane == line, col, 0), axis=0, keepdims=True)
    earlier = jnp.where((row == col) & (line < lane), 1, 0)
    rank = jnp.sum(earlier, axis=0, keepdims=True)
    cells = nx * ne
    slot = lax.broadcasted_iota(jnp.int32, (cells, rows), 0)
    swapped = lax.rem(slot, ne) * nx + slot // ne
    pick0 = one_hot((swapped == row) & (rank == 0))
    pick1 = one_hot((slot == row) & (rank == 1))
    here = lax.broadcasted_iota(jnp.int32, (cells, cells), 0)
    there = lax.broadcasted_iota(jnp.int32, (cells, cells), 1)
    to_ex = one_hot(there == lax.rem(here, nx) * ne + here // nx)
    to_xe = one_hot(there == lax.rem(here, ne) * nx + here // ne)

    with jax.named_scope("moe_norm"):
        widened = mixed_ref[...].astype(F32)
        scale = lax.rsqrt(jnp.mean(widened * widened, axis=-1, keepdims=True) + EPS)
        normed[...] = (widened * scale * moe_gain_ref[...]).astype(BF16)

    part = width // CHUNKS
    tile = 512

    def tiles(chunk, body):
        def step(i, carry):
            body(pl.ds(pl.multiple_of(chunk * part + i * tile, tile), tile))
            return carry

        lax.fori_loop(0, part // tile, step, 0)

    def put(ref, cols, value):
        ref[:, :, cols] = value.reshape(ref.shape[0], ref.shape[1], tile).astype(BF16)

    def get(ref, cols):
        return ref[:, :, cols].astype(F32).reshape(cells, tile).astype(BF16)

    def send(src, dst, k, chunk):
        n = dst.shape[0]
        me = x if n == nx else e
        cols = pl.ds(chunk * part, part)
        for i in range(1, n):
            to = lax.rem(me + i, n)
            pltpu.make_async_remote_copy(
                src.at[to, :, cols], dst.at[me, :, cols], msend.at[k, chunk], mrecv.at[k, chunk],
                device_id=(g, e, to) if n == nx else (g, to, x), device_id_type=MESH,
            ).start()
        dst[me, :, cols] = src[me, :, cols]

    def arrive(dst, k, chunk):
        ref = dst.at[pl.ds(0, dst.shape[0] - 1), :, pl.ds(chunk * part, part)]
        pltpu.make_async_copy(ref, ref, msend.at[k, chunk]).wait()
        pltpu.make_async_copy(ref, ref, mrecv.at[k, chunk]).wait()

    def two_phases(base, a0, m0, n0, d0, a1, m1, n1, d1, order0, order1, fill):
        for chunk in range(CHUNKS):
            with jax.named_scope("fill"):
                fill(chunk)
            send(a0, m0, base, chunk)
            send(a1, m1, base + 1, chunk)
        for chunk in range(CHUNKS):
            with jax.named_scope("wait_first"):
                arrive(m0, base, chunk)
            with jax.named_scope("permute"):
                tiles(chunk, lambda cols: put(n0, cols, dot(order0, get(m0, cols))))
            send(n0, d0, base + 2, chunk)
            with jax.named_scope("wait_first"):
                arrive(m1, base + 1, chunk)
            with jax.named_scope("permute"):
                tiles(chunk, lambda cols: put(n1, cols, dot(order1, get(m1, cols))))
            send(n1, d1, base + 3, chunk)

    def scatter(chunk):
        def body(cols):
            put(s0, cols, dot(pick0, normed[:, cols]))
            put(s1, cols, dot(pick1, normed[:, cols]))

        tiles(chunk, body)

    two_phases(0, s0, r0, t0, q0, s1, r1, t1, q1, to_ex, to_xe, scatter)
    with jax.named_scope("weights"):
        for weight in weights:
            weight.wait()

    ff = gate.shape[1]
    ftile = 256
    for chunk in range(CHUNKS):
        with jax.named_scope("wait_second"):
            arrive(q0, 2, chunk)
            arrive(q1, 3, chunk)
        with jax.named_scope("inner"):
            cols = pl.ds(chunk * part, part)
            tokens = jnp.concatenate(
                [q[:, :, cols].astype(F32).reshape(cells, part).astype(BF16) for q in (q0, q1)], axis=0
            )
            if chunk == 0:
                gate_acc[...] = dot(tokens, gate[cols, :])
                up_acc[...] = dot(tokens, up[cols, :])
            else:
                gate_acc[...] += dot(tokens, gate[cols, :])
                up_acc[...] += dot(tokens, up[cols, :])
    with jax.named_scope("silu"):
        hid[...] = (jax.nn.silu(gate_acc[...]) * up_acc[...]).astype(BF16)

    def outer(chunk):
        def body(cols):
            put(o0, cols, dot(hid[pl.ds(0, cells), :], down[:, cols]))
            put(o1, cols, dot(hid[pl.ds(cells, cells), :], down[:, cols]))

        tiles(chunk, body)

    two_phases(4, o0, b0, c0, f0, o1, b1, c1, f1, to_xe, to_ex, outer)
    for chunk in range(CHUNKS):
        with jax.named_scope("wait_second"):
            arrive(f0, 6, chunk)
            arrive(f1, 7, chunk)

        def combine(cols):
            moe = dot_t(pick0, get(f0, cols)) + dot_t(pick1, get(f1, cols))
            out_ref[:, cols] = (mixed_ref[:, cols].astype(F32) + moe).astype(BF16)

        with jax.named_scope("combine"):
            tiles(chunk, combine)
    for ring in kv_x + kv_y + ow_x + near + rest + straight:
        ring.finish()


def layer(prompt, hidden, queries, gain, moe_gain, lengths, ids, kvw, ow, expert_table, gate, up, down):
    nx, ne = lax.axis_size("rep"), lax.axis_size("ep")
    rows, width = hidden.shape
    count = prompt.shape[0]
    plen = count // GROUP_PROMPTS
    keys = plen * ne
    ff = gate.shape[1]
    vmem, any_ = pl.BlockSpec(memory_space=pltpu.VMEM), pl.BlockSpec(memory_space=pl.ANY)
    smem = pl.BlockSpec(memory_space=pltpu.SMEM)
    cols = queries.shape[1]
    table = expert_table.reshape(-1, 128)
    sem = pltpu.SemaphoreType.DMA
    xe = pltpu.VMEM((nx, ne, width), BF16)
    ex = pltpu.VMEM((ne, nx, width), BF16)
    return pl.pallas_call(
        functools.partial(layer_kernel, nx, ne),
        out_shape=jax.ShapeDtypeStruct((rows, width), BF16),
        in_specs=[any_] * 3 + [vmem] * 2 + [smem] * 2 + [vmem] + [any_] * 6,
        out_specs=vmem,
        scratch_shapes=[
            pltpu.VMEM(prompt.shape, BF16),
            pltpu.VMEM(hidden.shape, BF16),
            pltpu.VMEM(queries.shape, BF16),
            pltpu.VMEM((nx,) + kvw.shape, BF16),
            pltpu.VMEM((nx,) + ow.shape, BF16),
            pltpu.VMEM(table.shape, jnp.int32),
            pltpu.VMEM((rows, 128), jnp.int32),
            pltpu.VMEM((rows, width), BF16),
            pltpu.VMEM((count, width), BF16),
            pltpu.VMEM((2, queries.shape[0], HEAD_DIM), F32),
            pltpu.VMEM((nx, rows, cols), BF16),
            pltpu.VMEM((KEY_VALUE_HEADS, 2, rows, HEAD_DIM), BF16),
            pltpu.VMEM((nx, 2, rows, HEAD_DIM), BF16),
            pltpu.VMEM((GROUP_PROMPTS, 2, plen, HEAD_DIM), BF16),
            pltpu.VMEM((2, ne // 2, 2, plen, HEAD_DIM), BF16),
            pltpu.VMEM((keys, HEAD_DIM), F32),
            pltpu.VMEM((keys, HEAD_DIM), BF16),
            pltpu.VMEM((keys, HEAD_DIM), BF16),
            pltpu.VMEM((nx, rows, cols), BF16),
            pltpu.VMEM((nx, rows, cols), BF16),
            pltpu.VMEM((rows, width), BF16),
            pltpu.VMEM((rows // 16, 32 * nx, 1), F32),
            pltpu.VMEM((rows // 16, 32 * nx, 1), F32),
            pltpu.VMEM((rows // 16, 32 * nx, HEAD_DIM), F32),
            pltpu.VMEM(gate.shape, BF16), pltpu.VMEM(up.shape, BF16), pltpu.VMEM(down.shape, BF16),
            pltpu.VMEM((rows, width), BF16), pltpu.VMEM((2 * nx * ne, ff), BF16),
            pltpu.VMEM((2 * nx * ne, ff), F32), pltpu.VMEM((2 * nx * ne, ff), F32),
            xe, ex, xe, ex, ex, xe, ex, xe, ex, xe, ex, xe, xe, ex, xe, ex,
            sem((8,)), sem((3,)), sem((22,)), sem((22, 4)), sem((5,)), sem((5,)), sem((4,)), sem((4,)),
            sem((8, CHUNKS)), sem((8, CHUNKS)),
        ],
        compiler_params=pltpu.CompilerParams(
            collective_id=0, has_side_effects=True, vmem_limit_bytes=67043328
        ),
        name="layer",
    )(
        prompt, hidden, queries, gain.reshape(1, width), moe_gain.reshape(1, width), lengths,
        ids.reshape(rows), ids.reshape(1, rows), kvw, ow, table, gate, up, down,
    )


def local(
    prompt_hidden,
    decode_hidden,
    queries,
    attn_gain,
    key_value_weight,
    out_weight,
    moe_gain,
    gate_weight,
    up_weight,
    down_weight,
    expert_table,
    token_ids,
    prompt_lengths,
):
    width = decode_hidden.shape[2]
    out = layer(
        prompt_hidden.reshape(-1, width),
        decode_hidden.reshape(-1, width),
        queries.reshape(-1, queries.shape[2]),
        attn_gain,
        moe_gain,
        prompt_lengths,
        token_ids,
        key_value_weight,
        out_weight,
        expert_table,
        gate_weight[0],
        up_weight[0],
        down_weight[0],
    )
    return out.reshape(decode_hidden.shape)


def solution(mesh):
    placed = (
        P("groups", "ep", None),
        P(("groups", "ep"), "rep", None),
        P(("groups", "ep"), None, "rep"),
        P(),
        P(None, "rep"),
        P("rep", None),
        P(),
        P(("ep", "rep"), None, None),
        P(("ep", "rep"), None, None),
        P(("ep", "rep"), None, None),
        P(),
        P("ep", "rep"),
        P("groups"),
    )
    return jax.shard_map(
        local,
        mesh=mesh,
        in_specs=placed,
        out_specs=P(("groups", "ep"), "rep", None),
        check_vma=False,
    )
```

```python
import functools
import math

import jax
import jax.numpy as jnp
from jax import lax
from jax.experimental import pallas as pl
from jax.experimental.pallas import tpu as pltpu
from jax.sharding import PartitionSpec as P

HEAD_DIM = 128
QUERY_HEADS = 16
KEY_VALUE_HEADS = 4
GROUP_PROMPTS = 4
CAP = 2

EPS = 1e-06
THETA = 1000000.0
MESH = pl.DeviceIdType.MESH
F32 = jnp.float32
BF16 = jnp.bfloat16


def dot(a, b):
    return jnp.dot(a, b, preferred_element_type=F32)


def dot_t(a, b):
    return lax.dot_general(a, b, (((0,), (0,)), ((), ())), preferred_element_type=F32)


def one_hot(hit):
    return jnp.where(hit, 1.0, 0.0).astype(BF16)


SHARED_ROWS = 1024
DIRECT = 512
FAR = 4
CHUNKS = 4


def layer_kernel(
    nx, ne, prompt_hbm, hidden_hbm, query_hbm, gain_ref, moe_gain_ref, lengths_ref, ids_ref, idrow_ref,
    kvw_hbm, ow_hbm, table_hbm, gate_hbm, up_hbm, down_hbm, out_ref,
    prompt_ref, hidden_ref, query_ref,
    kvw, ow, table, picked, hn, pn, qf, qt, skv, dkv, spk, pkv, pf, kp, vp, att, full, mixed_ref, top_p, total_p, summed_p,
    gate, up, down, normed, hid, gate_acc, up_acc,
    s0, s1, r0, r1, t0, t1, q0, q1, o0, o1, b0, b1, c0, c1, f0, f1,
    lsem, wsem, ring_send, ring_recv, dd_send, dd_recv, xs, xr, msend, mrecv,
):
    e, x, g = lax.axis_index("ep"), lax.axis_index("rep"), lax.axis_index("groups")
    ny = ne // 2
    y, c = e // 2, lax.rem(e, 2)
    rows, width = hidden_hbm.shape
    shared = SHARED_ROWS
    piece = shared // ne
    sub = (width - shared) // 4
    orow = ow.shape[1] // ne
    half = (width - DIRECT) // 2
    lines = ow.shape[1] // 4
    spread_cols = pl.ds(DIRECT, width - DIRECT)
    plen = prompt_hbm.shape[0] // GROUP_PROMPTS
    own_prompt = e // (ne // GROUP_PROMPTS)
    seqs = 16

    def sub_rows(core, s):
        return pl.ds(pl.multiple_of(shared + core * (2 * sub) + s * sub, 16), sub)

    def piece_rows(k, size, unit):
        return pl.ds(pl.multiple_of(k * unit, 16), size)

    loads = [
        pltpu.make_async_copy(
            kvw_hbm.at[pl.ds(shared, width - shared)], kvw.at[x, pl.ds(shared, width - shared)], lsem.at[0]
        ),
        pltpu.make_async_copy(
            kvw_hbm.at[piece_rows(e, piece, piece)], kvw.at[x, piece_rows(e, piece, piece)], lsem.at[1]
        ),
        pltpu.make_async_copy(
            ow_hbm.at[piece_rows(e, orow, orow), spread_cols],
            ow.at[FAR, piece_rows(e, orow, orow), spread_cols],
            lsem.at[2],
        ),
        pltpu.make_async_copy(ow_hbm.at[:, pl.ds(0, DIRECT)], ow.at[FAR, :, pl.ds(0, DIRECT)], lsem.at[7]),
    ]
    late = [
        pltpu.make_async_copy(hidden_hbm, hidden_ref, lsem.at[3]),
        pltpu.make_async_copy(prompt_hbm, prompt_ref, lsem.at[4]),
        pltpu.make_async_copy(query_hbm, query_ref, lsem.at[5]),
        pltpu.make_async_copy(table_hbm, table, lsem.at[6]),
    ]
    weights = [
        pltpu.make_async_copy(gate_hbm, gate, wsem.at[0]),
        pltpu.make_async_copy(up_hbm, up, wsem.at[1]),
        pltpu.make_async_copy(down_hbm, down, wsem.at[2]),
    ]
    for load in loads + late:
        load.start()

    sibling = (g, 2 * y + 1 - c, x)

    def at_x(k):
        return (g, e, lax.rem(x + k + nx, nx))

    def at_y(k):
        return (g, 2 * lax.rem(y + k + ny, ny) + c, x)

    barrier = pltpu.get_barrier_semaphore()
    for i in range(1, nx):
        pl.semaphore_signal(barrier, inc=1, device_id=at_x(i), device_id_type=MESH)
    for i in range(1, ne):
        peer = (g, lax.rem(e + i, ne), x)
        pl.semaphore_signal(barrier, inc=1, device_id=peer, device_id_type=MESH)

    class Ring:
        def __init__(self, number, along, sign, hops, place, total, mate):
            self.along, self.sign, self.hops, self.place = along, sign, hops, place
            self.number, self.total, self.mate = number, total, mate

        def origin(self, h):
            me, n = (x, nx) if self.along == "x" else (y, ny)
            return lax.rem(me - self.sign * h + n, n)

        def at(self, h):
            return self.place(self.origin(h), (FAR - self.sign * h) % (2 * FAR))

        def go(self, h):
            ref = self.at(h)
            there = self.place(self.origin(h), (FAR - self.sign * (h + 1)) % (2 * FAR))
            to = at_x(self.sign) if self.along == "x" else at_y(self.sign)
            pltpu.make_async_remote_copy(
                ref, there, ring_send.at[self.number], ring_recv.at[self.number, h],
                device_id=to, device_id_type=MESH,
            ).start()

        def event(self, h):
            if h > self.hops:
                return
            ref = self.at(h)
            pltpu.make_async_copy(ref, ref, ring_recv.at[self.number, h - 1]).wait()
            if h < self.hops:
                self.go(h)
            if self.mate is not None:
                to_mate(ref, self.mate)

        def finish(self):
            ref = self.total(self.hops)
            pltpu.make_async_copy(ref, ref, ring_send.at[self.number]).wait()

    def to_mate(ref, k):
        pltpu.make_async_remote_copy(
            ref, ref, dd_send.at[k], dd_recv.at[k], device_id=sibling, device_id_type=MESH
        ).start()

    def mate_done(ref, k):
        pltpu.make_async_copy(ref, ref, dd_send.at[k]).wait()
        pltpu.make_async_copy(ref, ref, dd_recv.at[k]).wait()

    def pair(base, along, more, place, total, mate):
        return [
            Ring(base, along, 1, 4 if more else 3, place, total, mate),
            Ring(base + 1, along, -1, 3 if more else 4, place, total, mate),
        ]

    def kv_pair(base, s):
        return pair(
            base, "x", s == 0,
            lambda j, i: kvw.at[j, sub_rows(c, s)],
            lambda n: kvw.at[pl.ds(0, n), pl.ds(0, sub)],
            0,
        )

    def kv_spread(base, s):
        slices = pl.ds(4 * s, 4)
        return pair(
            base, "y", s == 0,
            lambda k, i: kvw.at[slices, piece_rows(2 * k + c, piece, piece)],
            lambda n: kvw.at[slices, pl.ds(0, n * piece)],
            3,
        )

    def spread_pair(base, s):
        return pair(
            base, "x", s == 0,
            lambda j, i: ow.at[i, piece_rows(e, orow, orow), pl.ds(DIRECT + s * half, half)],
            lambda n: ow.at[pl.ds(0, n), pl.ds(0, orow), pl.ds(0, half)],
            None,
        )

    def ow_pair(base, more, first, n_slices):
        slices = pl.ds(first, n_slices)
        return pair(
            base, "y", more,
            lambda k, i: ow.at[
                slices, piece_rows(2 * k + c, orow, orow), spread_cols
            ],
            lambda n: ow.at[slices, pl.ds(0, n * orow), spread_cols],
            1,
        )

    def direct_pair(base, s):
        return pair(
            base, "x", s == 0,
            lambda j, i: ow.at[
                i, pl.ds(pl.multiple_of(c * (2 * lines) + s * lines, 16), lines), pl.ds(0, DIRECT)
            ],
            lambda n: ow.at[pl.ds(0, n), pl.ds(0, lines), pl.ds(0, DIRECT)],
            4,
        )

    straight = direct_pair(18, 0) + direct_pair(20, 1)
    kv_x = kv_pair(0, 0) + kv_pair(2, 1)
    kv_y = kv_spread(14, 0) + kv_spread(16, 1)
    ow_x = spread_pair(4, 0) + spread_pair(6, 1)
    near = ow_pair(8, True, FAR - 1, 3)
    rest = ow_pair(10, False, 0, FAR - 1) + ow_pair(12, True, FAR + 2, nx - FAR - 2)

    def events(rings, h):
        for ring in rings:
            ring.event(h)

    def begin(rings, slices):
        for ring in rings:
            ring.go(0)
        to_mate(ow.at[slices, piece_rows(e, orow, orow), spread_cols], 1)

    def normalised(ref, out):
        widened = ref[...].astype(F32)
        scale = lax.rsqrt(jnp.mean(widened * widened, axis=-1, keepdims=True) + EPS)
        out[...] = (widened * scale * gain_ref[...]).astype(BF16)

    with jax.named_scope("enter"):
        for load in loads:
            load.wait()
        pl.semaphore_wait(barrier, nx + ne - 2)

    own_piece = piece_rows(e, piece, piece)
    for i in range(1, nx):
        ref = kvw.at[x, own_piece]
        pltpu.make_async_remote_copy(
            ref, ref, xs.at[0], xr.at[0], device_id=at_x(i), device_id_type=MESH
        ).start()
    for ring in kv_x:
        ring.go(0)
    for load in late:
        load.wait()
    normalised(hidden_ref, hn)
    with jax.named_scope("spread_wait"):
        ref = kvw.at[pl.ds(0, nx - 1), pl.ds(0, piece)]
        pltpu.make_async_copy(ref, ref, xs.at[0]).wait()
        pltpu.make_async_copy(ref, ref, xr.at[0]).wait()
    for ring in kv_y:
        ring.go(0)
    for ring in ow_x:
        ring.go(0)
    for s in range(2):
        to_mate(kvw.at[pl.ds(4 * s, 4), own_piece], 3)
    for h in range(1, 5):
        with jax.named_scope(f"kv_x#h={h}"):
            events(kv_x, h)
        if h == 4:
            with jax.named_scope("ow_x#h=4"):
                events(ow_x, 4)
            begin(rest, pl.ds(0, FAR - 1))
            to_mate(ow.at[pl.ds(FAR + 2, nx - FAR - 2), piece_rows(e, orow, orow), spread_cols], 1)
        with jax.named_scope(f"kv_y#h={h}"):
            events(kv_y, h)
        if h == 3:
            begin(near, pl.ds(FAR - 1, 3))
            for ring in straight:
                ring.go(0)
        if h < 4:
            with jax.named_scope(f"ow_x#h={h}"):
                events(ow_x, h)
        if h == 1:
            normalised(prompt_ref, pn)
            for k in range(2):
                qf[k] = query_ref[:, pl.ds(k * HEAD_DIM, HEAD_DIM)].astype(F32)
            for weight in weights:
                weight.start()
        if h == 2:
            for t in range(nx):
                for k in range(2):
                    cols = pl.ds(k * HEAD_DIM, HEAD_DIM)
                    qt[t, :, cols] = qf[k, pl.ds(t, rows, stride=nx), :].astype(BF16)
    with jax.named_scope("kv_mate"):
        mate_done(kvw.at[pl.ds(0, nx - 1), pl.ds(0, 2 * sub)], 0)
        mate_done(kvw.at[pl.ds(0, nx), pl.ds(0, ny * piece)], 3)

    length = lengths_ref[own_prompt]
    half_dim = HEAD_DIM // 2

    def turns(count, positions):
        lane = lax.broadcasted_iota(jnp.int32, (count, HEAD_DIM), 1)
        freq = jnp.exp(lax.rem(lane, half_dim).astype(F32) * (-2.0 * math.log(THETA) / HEAD_DIM))
        angles = positions.astype(F32) * freq
        sine = jnp.sin(angles)
        return jnp.cos(angles), jnp.where(lane < half_dim, -sine, sine)

    def turned(keys, cosine, sine):
        return keys * cosine + pltpu.roll(keys, half_dim, 1) * sine

    cosine, sine = turns(8, jnp.full((8, HEAD_DIM), length + x, jnp.int32))
    cosine, sine = cosine[0:1], sine[0:1]
    def own_kv(head):
        skv[head, 0] = turned(dot(hn[...], kvw[2 * head]), cosine, sine).astype(BF16)
        skv[head, 1] = dot(hn[...], kvw[2 * head + 1]).astype(BF16)

    def send_kv(head, to):
        pltpu.make_async_remote_copy(
            skv.at[head], dkv.at[x], xs.at[1], xr.at[1], device_id=(g, e, to), device_id_type=MESH
        ).start()

    with jax.named_scope("straight#h=1"):
        events(straight, 1)
    with jax.named_scope("own_kv"):
        for i in (2, 1, 3, 0):
            head = lax.rem(x // 2 + i, KEY_VALUE_HEADS)
            own_kv(head)
            if i:
                send_kv(head, 2 * head)
                send_kv(head, 2 * head + 1)
            else:
                send_kv(head, x + 1 - 2 * lax.rem(x, 2))
    dkv[x] = skv[x // 2]

    count = GROUP_PROMPTS * plen
    line = lax.broadcasted_iota(jnp.int32, (count, HEAD_DIM), 0)
    pcos, psin = turns(count, e * plen + lax.rem(line, plen))
    head = x // 2
    with jax.named_scope("prompt_kv"):
        pkey = turned(dot(pn[...], kvw[2 * head]), pcos, psin)
        pval = dot(pn[...], kvw[2 * head + 1])
    spk[:, 0] = pkey.reshape(GROUP_PROMPTS, plen, HEAD_DIM).astype(BF16)
    spk[:, 1] = pval.reshape(GROUP_PROMPTS, plen, HEAD_DIM).astype(BF16)
    per = ny // GROUP_PROMPTS
    for i in range(1, ny):
        to = lax.rem(y + i, ny)
        pltpu.make_async_remote_copy(
            spk.at[to // per], pkv.at[c, y], xs.at[2], xr.at[2],
            device_id=(g, 2 * to + c, x), device_id_type=MESH,
        ).start()
    pkv[c, y] = spk[y // per]
    with jax.named_scope("near#h=1"):
        events(near, 1)

    def look(i, carry):
        at = lax.div(ids_ref[i], 128)
        picked[pl.ds(i, 1), :] = table[pl.ds(at, 1), :]
        return carry

    with jax.named_scope("look"):
        lax.fori_loop(0, rows, look, 0)
    with jax.named_scope("prompt_wait"):
        ref = pkv.at[0, pl.ds(0, ny - 1)]
        pltpu.make_async_copy(ref, ref, xs.at[2]).wait()
        pltpu.make_async_copy(ref, ref, xr.at[2]).wait()
        to_mate(pkv.at[c], 2)
        mate_done(pkv.at[0], 2)
    for k in range(2):
        for core in range(2):
            for row in range(ny):
                start = (2 * row + core) * plen
                pf[pl.ds(start, plen), :] = pkv[core, row, k].astype(F32)
        (kp if k == 0 else vp)[...] = pf[...].astype(BF16)

    keys = kp.shape[0]
    block = 2 * nx * seqs
    scale = HEAD_DIM ** (-0.5)
    valid = lax.broadcasted_iota(jnp.int32, (block, keys), 1) < length
    r = lax.rem(lax.broadcasted_iota(jnp.int32, (block, nx * seqs), 0), nx * seqs)
    k = lax.broadcasted_iota(jnp.int32, (block, nx * seqs), 1)
    own = (lax.rem(r, seqs) == lax.rem(k, seqs)) & (k // seqs <= r // seqs)

    def nt(a, b):
        return lax.dot_general(a, b, (((1,), (1,)), ((), ())), preferred_element_type=F32)

    def asked(pick):
        return jnp.concatenate(
            [qt[:, pick, pl.ds(h * HEAD_DIM, HEAD_DIM)].reshape(nx * seqs, HEAD_DIM) for h in range(2)], axis=0
        )

    def twice(body, i, carry):
        return body(2 * i + 1, body(2 * i, carry))

    def attend_prompt(j, carry):
        pick = pl.ds(pl.multiple_of(j * seqs, seqs), seqs)
        scores = jnp.where(valid, nt(asked(pick), kp[...]) * scale, -1e30)
        top = jnp.max(scores, axis=1, keepdims=True)
        weight = jnp.where(valid, jnp.exp(scores - top), 0.0)
        top_p[j] = top
        total_p[j] = jnp.sum(weight, axis=1, keepdims=True)
        summed_p[j] = dot(weight.astype(BF16), vp[...])
        return carry

    def attend(j, carry):
        pick = pl.ds(pl.multiple_of(j * seqs, seqs), seqs)
        scores = nt(asked(pick), dkv[:, 0, pick].reshape(nx * seqs, HEAD_DIM)) * scale
        scores = jnp.where(own, scores, -1e30)
        top = jnp.maximum(top_p[j], jnp.max(scores, axis=1, keepdims=True))
        weight = jnp.where(own, jnp.exp(scores - top), 0.0)
        decay = jnp.exp(top_p[j] - top)
        total = total_p[j] * decay + jnp.sum(weight, axis=1, keepdims=True)
        summed = summed_p[j] * decay
        summed = summed + dot(weight.astype(BF16), dkv[:, 1, pick].reshape(nx * seqs, HEAD_DIM))
        result = (summed / total).astype(BF16)
        for h in range(2):
            att[:, pick, pl.ds(h * HEAD_DIM, HEAD_DIM)] = result[h * nx * seqs:(h + 1) * nx * seqs].reshape(
                nx, seqs, HEAD_DIM
            )
        return carry

    with jax.named_scope("rest#h=1"):
        events(rest, 1)
    with jax.named_scope("attend_prompt"):
        lax.fori_loop(0, rows // seqs // 2, functools.partial(twice, attend_prompt), 0)
    with jax.named_scope("straight#h=2"):
        events(straight, 2)
    with jax.named_scope("near#h=2"):
        events(near, 2)
    with jax.named_scope("kv_wait"):
        ref = dkv.at[pl.ds(0, nx - 1)]
        pltpu.make_async_copy(ref, ref, xs.at[1]).wait()
        pltpu.make_async_copy(ref, ref, xr.at[1]).wait()
    with jax.named_scope("attend"):
        lax.fori_loop(0, rows // seqs // 2, functools.partial(twice, attend), 0)
    with jax.named_scope("straight#h=3"):
        events(straight, 3)
    for i in range(1, nx):
        to = lax.rem(x + i, nx)
        pltpu.make_async_remote_copy(
            att.at[to], full.at[x], xs.at[3], xr.at[3], device_id=(g, e, to), device_id_type=MESH
        ).start()
    full[x] = att[x]
    with jax.named_scope("near#h=3"):
        events(near, 3)
    with jax.named_scope("rest#h=2"):
        events(rest, 2)
    with jax.named_scope("near#h=4"):
        events(near, 4)
    with jax.named_scope("rest#h=3"):
        events(rest, 3)
    with jax.named_scope("straight#h=4"):
        events(straight, 4)
    with jax.named_scope("rest#h=4"):
        events(rest, 4)
    with jax.named_scope("full_wait"):
        ref = full.at[pl.ds(0, nx - 1)]
        pltpu.make_async_copy(ref, ref, xs.at[3]).wait()
        pltpu.make_async_copy(ref, ref, xr.at[3]).wait()
    with jax.named_scope("ow_mate"):
        mate_done(ow.at[pl.ds(0, nx), pl.ds(0, ny * orow), spread_cols], 1)
        mate_done(ow.at[pl.ds(0, nx - 1), pl.ds(0, 2 * lines), pl.ds(0, DIRECT)], 4)

    tile = 512

    def project(i, carry):
        cols = pl.ds(pl.multiple_of(i * tile, tile), tile)
        total = dot(full[x], ow[FAR, :, cols])
        for k in range(1, nx):
            total = total + dot(full[lax.rem(x + k, nx)], ow[(FAR + k) % nx, :, cols])
        mixed_ref[:, cols] = (hidden_ref[:, cols].astype(F32) + total).astype(BF16)
        return carry

    with jax.named_scope("project"):
        lax.fori_loop(0, width // tile, project, 0)
    lane = lax.broadcasted_iota(jnp.int32, (rows, rows), 1)
    line = lax.broadcasted_iota(jnp.int32, (rows, rows), 0)
    idcol = jnp.sum(jnp.where(lane == line, idrow_ref[...], 0), axis=1, keepdims=True)
    col = jnp.sum(jnp.where(lane == lax.rem(idcol, 128), picked[...], 0), axis=1, keepdims=True)
    row = jnp.sum(jnp.where(lane == line, col, 0), axis=0, keepdims=True)
    earlier = jnp.where((row == col) & (line < lane), 1, 0)
    rank = jnp.sum(earlier, axis=0, keepdims=True)
    cells = nx * ne
    slot = lax.broadcasted_iota(jnp.int32, (cells, rows), 0)
    swapped = lax.rem(slot, ne) * nx + slot // ne
    pick0 = one_hot((swapped == row) & (rank == 0))
    pick1 = one_hot((slot == row) & (rank == 1))
    here = lax.broadcasted_iota(jnp.int32, (cells, cells), 0)
    there = lax.broadcasted_iota(jnp.int32, (cells, cells), 1)
    to_ex = one_hot(there == lax.rem(here, nx) * ne + here // nx)
    to_xe = one_hot(there == lax.rem(here, ne) * nx + here // ne)

    with jax.named_scope("moe_norm"):
        widened = mixed_ref[...].astype(F32)
        scale = lax.rsqrt(jnp.mean(widened * widened, axis=-1, keepdims=True) + EPS)
        normed[...] = (widened * scale * moe_gain_ref[...]).astype(BF16)

    part = width // CHUNKS
    tile = 512

    def tiles(chunk, body):
        def step(i, carry):
            body(pl.ds(pl.multiple_of(chunk * part + i * tile, tile), tile))
            return carry

        lax.fori_loop(0, part // tile, step, 0)

    def put(ref, cols, value):
        ref[:, :, cols] = value.reshape(ref.shape[0], ref.shape[1], tile).astype(BF16)

    def get(ref, cols):
        return ref[:, :, cols].astype(F32).reshape(cells, tile).astype(BF16)

    def send(src, dst, k, chunk):
        n = dst.shape[0]
        me = x if n == nx else e
        cols = pl.ds(chunk * part, part)
        for i in range(1, n):
            to = lax.rem(me + i, n)
            pltpu.make_async_remote_copy(
                src.at[to, :, cols], dst.at[me, :, cols], msend.at[k, chunk], mrecv.at[k, chunk],
                device_id=(g, e, to) if n == nx else (g, to, x), device_id_type=MESH,
            ).start()
        dst[me, :, cols] = src[me, :, cols]

    def arrive(dst, k, chunk):
        ref = dst.at[pl.ds(0, dst.shape[0] - 1), :, pl.ds(chunk * part, part)]
        pltpu.make_async_copy(ref, ref, msend.at[k, chunk]).wait()
        pltpu.make_async_copy(ref, ref, mrecv.at[k, chunk]).wait()

    def two_phases(base, a0, m0, n0, d0, a1, m1, n1, d1, order0, order1, fill):
        for chunk in range(CHUNKS):
            with jax.named_scope("fill"):
                fill(chunk)
            send(a0, m0, base, chunk)
            send(a1, m1, base + 1, chunk)
        for chunk in range(CHUNKS):
            with jax.named_scope("wait_first"):
                arrive(m0, base, chunk)
            with jax.named_scope("permute"):
                tiles(chunk, lambda cols: put(n0, cols, dot(order0, get(m0, cols))))
            send(n0, d0, base + 2, chunk)
            with jax.named_scope("wait_first"):
                arrive(m1, base + 1, chunk)
            with jax.named_scope("permute"):
                tiles(chunk, lambda cols: put(n1, cols, dot(order1, get(m1, cols))))
            send(n1, d1, base + 3, chunk)

    def scatter(chunk):
        def body(cols):
            put(s0, cols, dot(pick0, normed[:, cols]))
            put(s1, cols, dot(pick1, normed[:, cols]))

        tiles(chunk, body)

    two_phases(0, s0, r0, t0, q0, s1, r1, t1, q1, to_ex, to_xe, scatter)
    with jax.named_scope("weights"):
        for weight in weights:
            weight.wait()

    ff = gate.shape[1]
    ftile = 256
    for chunk in range(CHUNKS):
        with jax.named_scope("wait_second"):
            arrive(q0, 2, chunk)
            arrive(q1, 3, chunk)
        with jax.named_scope("inner"):
            cols = pl.ds(chunk * part, part)
            tokens = jnp.concatenate(
                [q[:, :, cols].astype(F32).reshape(cells, part).astype(BF16) for q in (q0, q1)], axis=0
            )
            if chunk == 0:
                gate_acc[...] = dot(tokens, gate[cols, :])
                up_acc[...] = dot(tokens, up[cols, :])
            else:
                gate_acc[...] += dot(tokens, gate[cols, :])
                up_acc[...] += dot(tokens, up[cols, :])
    with jax.named_scope("silu"):
        hid[...] = (jax.nn.silu(gate_acc[...]) * up_acc[...]).astype(BF16)

    def outer(chunk):
        def body(cols):
            put(o0, cols, dot(hid[pl.ds(0, cells), :], down[:, cols]))
            put(o1, cols, dot(hid[pl.ds(cells, cells), :], down[:, cols]))

        tiles(chunk, body)

    two_phases(4, o0, b0, c0, f0, o1, b1, c1, f1, to_xe, to_ex, outer)
    for chunk in range(CHUNKS):
        with jax.named_scope("wait_second"):
            arrive(f0, 6, chunk)
            arrive(f1, 7, chunk)

        def combine(cols):
            moe = dot_t(pick0, get(f0, cols)) + dot_t(pick1, get(f1, cols))
            out_ref[:, cols] = (mixed_ref[:, cols].astype(F32) + moe).astype(BF16)

        with jax.named_scope("combine"):
            tiles(chunk, combine)
    for ring in kv_x + kv_y + ow_x + near + rest + straight:
        ring.finish()


def layer(prompt, hidden, queries, gain, moe_gain, lengths, ids, kvw, ow, expert_table, gate, up, down):
    nx, ne = lax.axis_size("rep"), lax.axis_size("ep")
    rows, width = hidden.shape
    count = prompt.shape[0]
    plen = count // GROUP_PROMPTS
    keys = plen * ne
    ff = gate.shape[1]
    vmem, any_ = pl.BlockSpec(memory_space=pltpu.VMEM), pl.BlockSpec(memory_space=pl.ANY)
    smem = pl.BlockSpec(memory_space=pltpu.SMEM)
    cols = queries.shape[1]
    table = expert_table.reshape(-1, 128)
    sem = pltpu.SemaphoreType.DMA
    xe = pltpu.VMEM((nx, ne, width), BF16)
    ex = pltpu.VMEM((ne, nx, width), BF16)
    return pl.pallas_call(
        functools.partial(layer_kernel, nx, ne),
        out_shape=jax.ShapeDtypeStruct((rows, width), BF16),
        in_specs=[any_] * 3 + [vmem] * 2 + [smem] * 2 + [vmem] + [any_] * 6,
        out_specs=vmem,
        scratch_shapes=[
            pltpu.VMEM(prompt.shape, BF16),
            pltpu.VMEM(hidden.shape, BF16),
            pltpu.VMEM(queries.shape, BF16),
            pltpu.VMEM((nx,) + kvw.shape, BF16),
            pltpu.VMEM((nx,) + ow.shape, BF16),
            pltpu.VMEM(table.shape, jnp.int32),
            pltpu.VMEM((rows, 128), jnp.int32),
            pltpu.VMEM((rows, width), BF16),
            pltpu.VMEM((count, width), BF16),
            pltpu.VMEM((2, queries.shape[0], HEAD_DIM), F32),
            pltpu.VMEM((nx, rows, cols), BF16),
            pltpu.VMEM((KEY_VALUE_HEADS, 2, rows, HEAD_DIM), BF16),
            pltpu.VMEM((nx, 2, rows, HEAD_DIM), BF16),
            pltpu.VMEM((GROUP_PROMPTS, 2, plen, HEAD_DIM), BF16),
            pltpu.VMEM((2, ne // 2, 2, plen, HEAD_DIM), BF16),
            pltpu.VMEM((keys, HEAD_DIM), F32),
            pltpu.VMEM((keys, HEAD_DIM), BF16),
            pltpu.VMEM((keys, HEAD_DIM), BF16),
            pltpu.VMEM((nx, rows, cols), BF16),
            pltpu.VMEM((nx, rows, cols), BF16),
            pltpu.VMEM((rows, width), BF16),
            pltpu.VMEM((rows // 16, 32 * nx, 1), F32),
            pltpu.VMEM((rows // 16, 32 * nx, 1), F32),
            pltpu.VMEM((rows // 16, 32 * nx, HEAD_DIM), F32),
            pltpu.VMEM(gate.shape, BF16), pltpu.VMEM(up.shape, BF16), pltpu.VMEM(down.shape, BF16),
            pltpu.VMEM((rows, width), BF16), pltpu.VMEM((2 * nx * ne, ff), BF16),
            pltpu.VMEM((2 * nx * ne, ff), F32), pltpu.VMEM((2 * nx * ne, ff), F32),
            xe, ex, xe, ex, ex, xe, ex, xe, ex, xe, ex, xe, xe, ex, xe, ex,
            sem((8,)), sem((3,)), sem((22,)), sem((22, 4)), sem((5,)), sem((5,)), sem((4,)), sem((4,)),
            sem((8, CHUNKS)), sem((8, CHUNKS)),
        ],
        compiler_params=pltpu.CompilerParams(
            collective_id=0, has_side_effects=True, vmem_limit_bytes=67043328
        ),
        name="layer",
    )(
        prompt, hidden, queries, gain.reshape(1, width), moe_gain.reshape(1, width), lengths,
        ids.reshape(rows), ids.reshape(1, rows), kvw, ow, table, gate, up, down,
    )


def local(
    prompt_hidden,
    decode_hidden,
    queries,
    attn_gain,
    key_value_weight,
    out_weight,
    moe_gain,
    gate_weight,
    up_weight,
    down_weight,
    expert_table,
    token_ids,
    prompt_lengths,
):
    width = decode_hidden.shape[2]
    out = layer(
        prompt_hidden.reshape(-1, width),
        decode_hidden.reshape(-1, width),
        queries.reshape(-1, queries.shape[2]),
        attn_gain,
        moe_gain,
        prompt_lengths,
        token_ids,
        key_value_weight,
        out_weight,
        expert_table,
        gate_weight[0],
        up_weight[0],
        down_weight[0],
    )
    return out.reshape(decode_hidden.shape)


def solution(mesh):
    placed = (
        P("groups", "ep", None),
        P(("groups", "ep"), "rep", None),
        P(("groups", "ep"), None, "rep"),
        P(),
        P(None, "rep"),
        P("rep", None),
        P(),
        P(("ep", "rep"), None, None),
        P(("ep", "rep"), None, None),
        P(("ep", "rep"), None, None),
        P(),
        P("ep", "rep"),
        P("groups"),
    )
    return jax.shard_map(
        local,
        mesh=mesh,
        in_specs=placed,
        out_specs=P(("groups", "ep"), "rep", None),
        check_vma=False,
    )
```
